256 devices in a mesh: dp: 32 (over z, y), mp: 8 (over x, core).
Axes of the slice: x: 4, y: 4, z: 8, core: 2. Of those that a mesh axis runs over, the one named last changes fastest.
Arguments:
- queries: bfloat16 [4096, 8192], P('dp', 'mp'), may hold values from -8 to 8
- tree_keys: bfloat16 [4096, 1024], P('dp', 'mp'), may hold values from -18 to 18
- tree_values: bfloat16 [4096, 1024], P('dp', 'mp'), may hold values from -6 to 6
- cache_keys: bfloat16 [64, 4096, 1024], P('dp', None, 'mp'), may hold values from -8 to 8
- cache_values: bfloat16 [64, 4096, 1024], P('dp', None, 'mp'), may hold values from -6 to 6
- cache_lens: int32 [64], P('dp'), may hold values from 1024 to 4096, as said below
- parents: int32 [64, 64], P('dp'), may hold values from -1 to 62, as said below
- accepted_nodes: int32 [64, 8], P('dp'), may hold values from 0 to 63, as said below
- residual: bfloat16 [4096, 8192], P('dp', 'mp'), may hold values from -1.796875 to 1.796875
- out_weight: bfloat16 [8192, 8192], P('mp', 'dp'), may hold values from -0.0625 to 0.0625
Outputs:
- tree_hidden: bfloat16 [4096, 8192], P('dp', 'mp')
- accepted_hidden: bfloat16 [512, 8192], P(None, 'mp')
The draws below stay inside these ranges and needn't reach their ends.
Inputs may be any that keep to these rules, and one draw needn't show every extreme that they name: parents[r, 0] = -1 and 0 <= parents[r, i] < i for i >= 1. accepted_nodes[r, 0] = 0, the nodes of a row increase, and parents[r, accepted_nodes[r, a + 1]] = accepted_nodes[r, a]. `cache_lens`: some request has exactly 4096 filled positions.
All inputs are finite; a program needn't handle non-finite values.
Results may differ from the reference program's by a relative error of at most 0.015.
Values may be sent and summed in bfloat16 or wider, within the bound.
A program may use at most 64 MiB of HBM per device.

```python
import math
import jax
import jax.numpy as jnp
from jax import lax

D = 8192
HEADS = 64
KV_HEADS = 8
HD = 128
NODES = 64
ACC = 8
CACHE = 4096
REQUESTS = 64
ROWS = 4096


def tree_shape(key):

    def one_tree(tree_key):
        chain_key, parent_key = jax.random.split(tree_key)
        shuffled = jax.random.permutation(chain_key, NODES - 1) + 1
        chain_nodes = jnp.sort(shuffled[:ACC - 1]).astype(jnp.int32)
        positions = jnp.arange(NODES, dtype=jnp.int32)
        parent_list = jax.random.randint(parent_key, (NODES,), 0, jnp.maximum(positions, 1)).astype(jnp.int32)
        parent_list = jnp.where(positions == 0, -1, parent_list)
        previous = jnp.concatenate([jnp.zeros((1,), jnp.int32), chain_nodes[:-1]])
        parent_list = parent_list.at[chain_nodes].set(previous)
        accepted = jnp.concatenate([jnp.zeros((1,), jnp.int32), chain_nodes])
        return (parent_list, accepted)
    request_keys = jax.random.split(jax.random.fold_in(key, 11), REQUESTS)
    return jax.vmap(one_tree)(request_keys)


def draw_parents(key, part):
    return tree_shape(key)[0].astype(jnp.int32)


def draw_accepted_nodes(key, part):
    return tree_shape(key)[1].astype(jnp.int32)


def draw_cache_lens(key, part):
    length_key, chosen_key = jax.random.split(jax.random.fold_in(key, 31))
    lengths = jax.random.randint(length_key, (REQUESTS,), CACHE // 4, CACHE + 1)
    chosen = jax.random.randint(chosen_key, (), 0, REQUESTS)
    return jnp.where(jnp.arange(REQUESTS) == chosen, CACHE, lengths).astype(jnp.int32)


def draw_cache_keys(key, part):
    shape = (REQUESTS, CACHE, KV_HEADS * HD)
    values = jax.random.normal(jax.random.fold_in(key, 1), shape, jnp.float32)
    return jnp.clip(values, -8.0, 8.0).astype(jnp.bfloat16)


def draw_queries(key, part):
    shape = (REQUESTS * NODES, HEADS * HD)
    values = 1.7 * jax.random.normal(jax.random.fold_in(key, 3), shape, jnp.float32)
    return jnp.clip(values, -8.0, 8.0).astype(jnp.bfloat16)


def block_levels(rng, extent, shards, low, top_value):
    def one(position, shards_of):
        draws = jax.random.uniform(jax.random.fold_in(jax.random.fold_in(rng, 6), position), (shards_of,), jnp.float32, low / len(shards), top_value / len(shards))
        return jnp.repeat(jnp.exp(draws), extent[position] // shards_of).reshape((-1,) + (1,) * (len(extent) - position - 1))

    loudness = one(*shards[0])
    for cut in shards[1:]:
        loudness = loudness * one(*cut)
    return loudness


def normal_values(stream_key, dims, deviation, reach, shards=(), kind=jnp.bfloat16):
    result = deviation * jax.random.normal(stream_key, dims, jnp.float32)
    if shards:
        result = result * block_levels(stream_key, dims, shards, -0.22, 0.18)
    return jnp.clip(result, -reach, reach).astype(kind)


def setup_inputs(seed: int = 0) -> dict:
    key_list = jax.random.split(jax.random.key(seed), 11)
    return {
        "queries": draw_queries(jax.random.fold_in(key_list[10], 71), 0),
        "tree_keys": normal_values(key_list[1], (ROWS, KV_HEADS * HD), 3.0, 18.0, ((0, 32), (1, 8))),
        "tree_values": normal_values(key_list[2], (ROWS, KV_HEADS * HD), 1.0, 6.0, ((0, 32), (1, 8))),
        "cache_keys": draw_cache_keys(jax.random.fold_in(key_list[10], 71), 0),
        "cache_values": normal_values(key_list[4], (REQUESTS, CACHE, KV_HEADS * HD), 1.0, 6.0, ((0, 32), (2, 8))),
        "cache_lens": draw_cache_lens(jax.random.fold_in(key_list[10], 71), 0),
        "parents": draw_parents(jax.random.fold_in(key_list[10], 71), 0),
        "accepted_nodes": draw_accepted_nodes(jax.random.fold_in(key_list[10], 71), 0),
        "residual": normal_values(key_list[8], (ROWS, D), 0.3, 1.796875, ((0, 32), (1, 8))),
        "out_weight": normal_values(key_list[9], (HEADS * HD, D), (HEADS * HD) ** -0.5, 0.0625, ((0, 8), (1, 32))),
    }


neg_large = -1e+30

def ancestry(parents):
    positions = jnp.arange(NODES, dtype=jnp.int32)
    parent_hot = (parents[:, :, None] == positions[None, None, :]).astype(jnp.float32)
    reached = parent_hot + jnp.eye(NODES, dtype=jnp.float32)[None]
    for squaring in range((NODES - 1).bit_length()):
        reached = jnp.minimum(jnp.einsum('rij,rjk->rik', reached, reached, precision=lax.Precision.HIGHEST), 1.0)
    return reached > 0.5

def reference(queries, tree_keys, tree_values, cache_keys, cache_values, cache_lens, parents, accepted_nodes, residual, out_weight):
    group_size = HEADS // KV_HEADS
    scale_factor = 1.0 / math.sqrt(HD)
    ancestor = ancestry(parents)
    query_grid = queries.reshape(REQUESTS, NODES, KV_HEADS, group_size, HD)
    tree_key_grid = tree_keys.reshape(REQUESTS, NODES, KV_HEADS, HD)
    tree_value_grid = tree_values.reshape(REQUESTS, NODES, KV_HEADS, HD)
    cache_key_grid = cache_keys.reshape(REQUESTS, CACHE, KV_HEADS, HD)
    cache_value_grid = cache_values.reshape(REQUESTS, CACHE, KV_HEADS, HD)

    def one_request(request_data):
        query_one, tkey_one, tvalue_one, ckey_one, cvalue_one, cache_length, mask_one = request_data
        query_float = query_one.astype(jnp.float32)
        cache_scores = jnp.einsum('nkgd,pkd->nkgp', query_float, ckey_one.astype(jnp.float32), precision=lax.Precision.HIGHEST) * scale_factor
        live_keys = jnp.arange(CACHE, dtype=jnp.int32) < cache_length
        cache_scores = jnp.where(live_keys[None, None, None, :], cache_scores, neg_large)
        tree_scores = jnp.einsum('nkgd,jkd->nkgj', query_float, tkey_one.astype(jnp.float32), precision=lax.Precision.HIGHEST) * scale_factor
        tree_scores = jnp.where(mask_one[:, None, None, :], tree_scores, neg_large)
        row_max = jnp.maximum(lax.optimization_barrier(jnp.max(cache_scores, axis=-1)), lax.optimization_barrier(jnp.max(tree_scores, axis=-1)))
        cache_weights = jnp.exp(cache_scores - row_max[..., None])
        tree_weights = jnp.exp(tree_scores - row_max[..., None])
        denominator = lax.optimization_barrier(jnp.sum(cache_weights, axis=-1)) + lax.optimization_barrier(jnp.sum(tree_weights, axis=-1))
        rounded_cache = lax.optimization_barrier(cache_weights.astype(jnp.bfloat16)).astype(jnp.float32)
        rounded_tree = lax.optimization_barrier(tree_weights.astype(jnp.bfloat16)).astype(jnp.float32)
        numerator = jnp.einsum('nkgp,pkd->nkgd', rounded_cache, cvalue_one.astype(jnp.float32), precision=lax.Precision.HIGHEST)
        numerator = numerator + jnp.einsum('nkgj,jkd->nkgd', rounded_tree, tvalue_one.astype(jnp.float32), precision=lax.Precision.HIGHEST)
        return (numerator / denominator[..., None]).astype(jnp.bfloat16).reshape(NODES, HEADS * HD)
    attended = lax.map(one_request, (query_grid, tree_key_grid, tree_value_grid, cache_key_grid, cache_value_grid, cache_lens, ancestor))
    attended = attended.reshape(REQUESTS * NODES, HEADS * HD)
    projected = jnp.dot(attended, out_weight, preferred_element_type=jnp.float32)
    tree_hidden = (residual.astype(jnp.float32) + projected).astype(jnp.bfloat16)
    picked_rows = (jnp.arange(REQUESTS, dtype=jnp.int32)[:, None] * NODES + accepted_nodes).reshape(-1)
    accepted_hidden = jnp.take(tree_hidden, picked_rows, axis=0)
    return (tree_hidden, accepted_hidden)
```

```python
import functools
import math

import jax
import jax.numpy as jnp
from jax import lax
from jax.experimental import pallas as pl
from jax.experimental.pallas import tpu as pltpu
from jax.sharding import PartitionSpec as P

F32, BF16 = jnp.float32, jnp.bfloat16
MESH = pl.DeviceIdType.MESH
Z, Y, X = 8, 4, 4
NODES, HD, GROUP = 64, 128, 8
SCALE = math.log2(math.e) / math.sqrt(HD)
NEG = -1e30
NT = (((1,), (1,)), ((), ()))
TN = (((0,), (0,)), ((), ()))
CHUNK = 2048
ROWS = 256
CACHE = 4096
OFFSET = (0, -1, 1, -2, 2, -3, 3, 4)
GROUPS = ((0, 0, 4), (1, 0, 4), (0, 4, 4), (1, 4, 4))


def kernel(
    lens, ints, q, tk, tv, k_hbm, v_hbm, res_hbm, w_hbm,
    hid_out, acc_out,
    kb, vb, m_s, l_s, acc_s, a_buf, b_buf, part, pair_in, pair, r1_in, r2_src, r2_in, red, fin, res,
    loc_sem, a_send, a_recv, b_send, b_recv, d_send, d_recv, r1_send, r1_recv, r2_send, r2_recv,
    t_send, t_recv, cz_send, cz_recv, cy_send, cy_recv,
):
    dp, m = lax.axis_index("dp"), lax.axis_index("mp")
    z, y = dp // Y, dp % Y
    x, c = m // 2, m % 2
    is_self = m == z

    def at_z(dz):
        return (((z + dz + Z) % Z) * Y + y, m)

    def at_y(dy):
        return (z * Y + (y + dy + Y) % Y, m)

    def at_x(dx):
        return (dp, ((x + dx + X) % X) * 2 + c)

    partner = (dp, x * 2 + (1 - c))

    barrier = pltpu.get_barrier_semaphore()

    def greet(peer):
        pl.semaphore_signal(barrier, inc=1, device_id=peer, device_id_type=MESH)

    for peer in [at_y(1), at_y(-1), at_z(1), at_z(-1), partner, at_x(1), at_x(-1)]:
        greet(peer)
    for dz in range(2, Z - 1):
        greet(at_z(dz))
    for other in range(8):

        @pl.when(jnp.logical_or(m != z, m != other))
        def _():
            greet((m * Y + y, other))

    local = []
    for i, (src, dst) in enumerate(
        [(k_hbm.at[0], kb.at[0]), (v_hbm.at[0], vb.at[0]), (w_hbm, b_buf.at[0]),
         (k_hbm.at[1], kb.at[1]), (v_hbm.at[1], vb.at[1]), (res_hbm, res)]
    ):
        local.append(pltpu.make_async_copy(src, dst, loc_sem.at[i]))
        local[-1].start()

    def remote(src, dst, send, recv, peer):
        return pltpu.make_async_remote_copy(
            src_ref=src, dst_ref=dst, send_sem=send, recv_sem=recv, device_id=peer, device_id_type=MESH
        )

    sub = lax.broadcasted_iota(jnp.int32, (128, 128), 0)
    lane = lax.broadcasted_iota(jnp.int32, (128, 128), 1)
    eye = jnp.where(sub == lane, 1.0, 0.0)
    reach = jnp.where(sub == ints[0:1, :], 1.0, 0.0) + eye
    for _ in range(6):
        step = reach.astype(BF16)
        reach = jnp.minimum(jnp.dot(step, step, preferred_element_type=F32), 1.0)
    reach = lax.dot_general(reach.astype(BF16), eye.astype(BF16), TN, preferred_element_type=F32)

    heads = ROWS // NODES

    def query_rows(r, b):
        return jnp.concatenate(
            [q[r * NODES:(r + 1) * NODES, h * HD:(h + 1) * HD] for h in range(b * heads, (b + 1) * heads)], axis=0
        )

    def attend(r):
        mask = reach[r * NODES:(r + 1) * NODES, :] > 0.5
        mask = jnp.concatenate([mask] * heads, axis=0)
        for b in range(512 // ROWS):
            rows = slice(b * ROWS, (b + 1) * ROWS)
            s = lax.dot_general(query_rows(r, b), tk[...], NT, preferred_element_type=F32) * SCALE
            s = jnp.where(mask, s, NEG)
            top = jnp.max(s, axis=1, keepdims=True)
            p = jnp.exp2(s - top)
            m_s[rows, :] = jnp.broadcast_to(top, (ROWS, 128))
            l_s[rows, :] = p
            acc_s[rows, :] = jnp.dot(p.astype(BF16), tv[...], preferred_element_type=F32)
        local[3 * r].wait()
        local[3 * r + 1].wait()
        count = lens[r]

        def body(j, carry):
            base = pl.multiple_of(j * CHUNK, CHUNK)
            keys = kb[r, pl.ds(base, CHUNK), :]
            values = vb[r, pl.ds(base, CHUNK), :]
            live = (lax.broadcasted_iota(jnp.int32, (1, CHUNK), 1) + base) < count
            bias = jnp.where(live, 0.0, NEG)
            for b in range(512 // ROWS):
                rows = slice(b * ROWS, (b + 1) * ROWS)
                s = lax.dot_general(query_rows(r, b), keys, NT, preferred_element_type=F32)
                s = s * SCALE + bias
                top = s[:, 0:128]
                for t in range(1, CHUNK // 128):
                    top = jnp.maximum(top, s[:, t * 128:(t + 1) * 128])
                old = m_s[rows, :]
                new = jnp.maximum(old, jnp.broadcast_to(jnp.max(top, axis=1, keepdims=True), (ROWS, 128)))
                rescale = jnp.exp2(old - new)
                m_s[rows, :] = new
                total = l_s[rows, :] * rescale
                rounded = []
                for t in range(CHUNK // 128):
                    p = jnp.exp2(s[:, t * 128:(t + 1) * 128] - new)
                    total = total + p
                    rounded.append(p.astype(BF16))
                l_s[rows, :] = total
                acc_s[rows, :] = acc_s[rows, :] * rescale + jnp.dot(
                    jnp.concatenate(rounded, axis=1), values, preferred_element_type=F32
                )
            return carry

        lax.fori_loop(0, CACHE // CHUNK, body, 0)
        for b in range(512 // ROWS):
            rows = slice(b * ROWS, (b + 1) * ROWS)
            total = jnp.sum(l_s[rows, :], axis=1, keepdims=True)
            out = (acc_s[rows, :] / total).astype(BF16)
            for h in range(heads):
                col = (b * heads + h) * HD
                a_buf[r, 0, :, col:col + HD] = out[h * NODES:(h + 1) * NODES, :]

    def a_copy(r, s, way):
        sign = 1 if way == 0 else -1
        src = 0 if s == 1 else 2 * (s - 1) - 1 + way
        if s < 4:
            dst, cut = 2 * s - 1 + way, slice(None)
        else:
            dst, cut = 7, slice(32 * way, 32 * way + 32)
        return remote(
            a_buf.at[r, src, cut], a_buf.at[r, dst, cut], a_send.at[r, s - 1, way], a_recv.at[r, s - 1, way], at_z(sign)
        )

    def a_go(r, s):
        for way in range(2):
            if s > 1:
                a_copy(r, s - 1, way).wait_recv()
            a_copy(r, s, way).start()

    def a_end(r):
        for way in range(2):
            a_copy(r, 4, way).wait_recv()

    def y_copies(view, send, recv):
        up, down = at_y(1), at_y(-1)
        plan = [(0, 3, 0, up), (0, 1, 1, down), (0, 3, 1, up), (0, 1, 0, down), (3, 2, 0, up), (1, 2, 1, down)]
        return [
            remote(view(src, half), view(dst, half), send.at[i], recv.at[i], peer)
            for i, (src, dst, half, peer) in enumerate(plan)
        ]

    b_copies = y_copies(lambda slot, half: b_buf.at[slot, half * 512:(half + 1) * 512], b_send, b_recv)

    def forward(copies):
        for i in range(2):
            copies[i].wait_recv()
            copies[4 + i].start()

    def span(group):
        r, p0, n = group
        start = (r * 8 + p0) * NODES
        return start, n * NODES

    def multiply(g):
        r, p0, n = GROUPS[g]
        start, size = span(GROUPS[g])
        left = a_buf[r, p0:p0 + n].reshape(size, 1024)
        for rel in range(Y):
            product = jnp.dot(left, b_buf[rel], preferred_element_type=F32).astype(BF16)
            part[2 * rel, start:start + size, :] = product[:, :128]
            part[2 * rel + 1, start:start + size, :] = product[:, 128:]
        pair_copy(g).start()

    def pair_copy(g):
        start, size = span(GROUPS[g])
        return remote(
            part.at[pl.ds((1 - c) * 4, 4), start:start + size], pair_in.at[:, start:start + size],
            d_send.at[g], d_recv.at[g], partner,
        )

    def r1_copy(g, way):
        start, size = span(GROUPS[g])
        half = slice(start + way * size // 2, start + (way + 1) * size // 2)
        return remote(
            pair.at[(x + 2) % X, half], r1_in.at[half], r1_send.at[g, way], r1_recv.at[g, way], at_x(1 - 2 * way)
        )

    def add_pair(g):
        start, size = span(GROUPS[g])
        rows = slice(start, start + size)
        pair_copy(g).wait_recv()
        for i in range(X):
            pair[i, rows, :] = (part[c * 4 + i, rows, :].astype(F32) + pair_in[i, rows, :].astype(F32)).astype(BF16)
        for way in range(2):
            r1_copy(g, way).start()

    def r2_copy(g, way):
        start, size = span(GROUPS[g])
        rows = slice(start, start + size)
        return remote(
            r2_src.at[way, rows], r2_in.at[way, rows], r2_send.at[g, way], r2_recv.at[g, way], at_x(1 - 2 * way)
        )

    def add_far(g):
        start, size = span(GROUPS[g])
        for way in range(2):
            r1_copy(g, way).wait_recv()
            near = (x + 1 - 2 * way + X) % X
            for half in range(2):
                rows = slice(start + half * size // 2, start + (half + 1) * size // 2)
                value = pair[near, rows, :]
                if half == way:
                    value = (value.astype(F32) + r1_in[rows, :].astype(F32)).astype(BF16)
                r2_src[way, rows, :] = value
            r2_copy(g, way).start()

    part_of = c * 4 + x
    own_slice = ((y + part_of // 2) % Y) * 2 + part_of % 2

    def t_copy(r, p):
        return remote(
            red.at[r * 8 + p], fin.at[own_slice, r], t_send.at[r, p], t_recv.at[r, own_slice],
            (((z + OFFSET[p] + Z) % Z) * Y + y, z),
        )

    def spread(g):
        r, p0, n = GROUPS[g]
        start, size = span(GROUPS[g])
        rows = slice(start, start + size)
        for way in range(2):
            r2_copy(g, way).wait_recv()
        total = pair[x, rows, :].astype(F32) + r2_in[0, rows, :].astype(F32) + r2_in[1, rows, :].astype(F32)
        red[r * 8 + p0:r * 8 + p0 + n] = total.astype(BF16).reshape(n, NODES, HD)
        for p in range(p0, p0 + n):
            if p == 0:

                @pl.when(jnp.logical_not(is_self))
                def _():
                    t_copy(r, 0).start()

                @pl.when(is_self)
                def _():
                    fin[own_slice, r] = red[r * 8]

            else:
                t_copy(r, p).start()

    def finish(r):
        rows = slice(r * NODES, (r + 1) * NODES)
        for i in range(8):

            @pl.when(jnp.logical_or(m != z, own_slice != i))
            def _():
                remote(red.at[0], fin.at[i, r], t_send.at[r, 0], t_recv.at[r, i], partner).wait_recv()

            cols = slice(i * HD, (i + 1) * HD)
            hid_out[rows, cols] = (res[rows, cols].astype(F32) + fin[i, r].astype(F32)).astype(BF16)

    pl.semaphore_wait(barrier, jnp.where(is_self, 19, 20))
    local[2].wait()
    for i in range(4):
        b_copies[i].start()
    attend(0)
    a_go(0, 1)
    attend(1)
    a_go(1, 1)
    a_go(0, 2)
    forward(b_copies)
    a_go(1, 2)
    a_go(0, 3)
    a_go(1, 3)
    for i in (2, 3, 4, 5):
        b_copies[i].wait_recv()
    multiply(0)
    a_go(0, 4)
    multiply(1)
    add_pair(0)
    a_go(1, 4)
    add_pair(1)
    add_far(0)
    a_end(0)
    multiply(2)
    add_far(1)
    spread(0)
    a_end(1)
    multiply(3)
    add_pair(2)
    spread(1)
    add_pair(3)
    add_far(2)
    add_far(3)
    spread(2)
    spread(3)
    local[5].wait()
    finish(0)
    finish(1)

    pick = jnp.where(sub == ints[1:2, :], 1.0, 0.0).astype(BF16)
    picked = lax.dot_general(pick, hid_out[...], TN, preferred_element_type=F32)
    acc_out[z, y] = picked[0:16].astype(BF16)

    def cz_copy(dz):
        return remote(acc_out.at[z, y], acc_out.at[z, y], cz_send.at[dz - 1], cz_recv.at[dz - 1], at_z(dz))

    for dz in (4, 3, 5, 2, 6, 1, 7):
        cz_copy(dz).start()
    for dz in range(1, Z):
        cz_copy(dz).wait_recv()

    def acc_view(slot, half):
        return acc_out.at[half * 4:(half + 1) * 4, (y + slot) % Y]

    up, down = at_y(1), at_y(-1)
    plan = [(0, 0, up), (0, 1, down), (0, 1, up), (0, 0, down), (3, 0, up), (1, 1, down)]
    cy_copies = [
        remote(acc_view(slot, half), acc_view(slot, half), cy_send.at[i], cy_recv.at[i], peer)
        for i, (slot, half, peer) in enumerate(plan)
    ]
    for i in range(4):
        cy_copies[i].start()
    forward(cy_copies)
    for i in (2, 3, 4, 5):
        cy_copies[i].wait_recv()

    for r in range(2):
        for s in range(1, 5):
            for way in range(2):
                a_copy(r, s, way).wait_send()
        for p in range(8):
            if p == 0:

                @pl.when(jnp.logical_not(is_self))
                def _():
                    t_copy(r, 0).wait_send()

            else:
                t_copy(r, p).wait_send()
    for g in range(len(GROUPS)):
        pair_copy(g).wait_send()
        for way in range(2):
            r1_copy(g, way).wait_send()
            r2_copy(g, way).wait_send()
    for copy in b_copies + cy_copies:
        copy.wait_send()
    for dz in range(1, Z):
        cz_copy(dz).wait_send()


def per_device(
    queries, tree_keys, tree_values, cache_keys, cache_values, cache_lens, parents, accepted_nodes, residual, out_weight
):
    base = jnp.arange(2, dtype=jnp.int32)[:, None] * NODES
    tree = jnp.where(parents < 0, -1, parents + base).reshape(1, 128)
    picks = jnp.pad((accepted_nodes + base).reshape(1, 16), ((0, 0), (0, 112)), constant_values=-1)
    ints = jnp.concatenate([tree, picks], axis=0)
    vmem = pl.BlockSpec(memory_space=pltpu.VMEM)
    smem = pl.BlockSpec(memory_space=pltpu.SMEM)
    hbm = pl.BlockSpec(memory_space=pl.ANY)
    sems = pltpu.SemaphoreType.DMA
    groups = len(GROUPS)
    hidden, accepted = pl.pallas_call(
        kernel,
        out_shape=(
            jax.ShapeDtypeStruct((128, 1024), BF16),
            jax.ShapeDtypeStruct((Z, Y, 16, 1024), BF16),
        ),
        in_specs=[smem, vmem, vmem, vmem, vmem, hbm, hbm, hbm, hbm],
        out_specs=(vmem, vmem),
        scratch_shapes=[
            pltpu.VMEM((2, CACHE, HD), BF16),
            pltpu.VMEM((2, CACHE, HD), BF16),
            pltpu.VMEM((512, 128), F32),
            pltpu.VMEM((512, 128), F32),
            pltpu.VMEM((512, 128), F32),
            pltpu.VMEM((2, 8, NODES, 1024), BF16),
            pltpu.VMEM((Y, 1024, 256), BF16),
            pltpu.VMEM((8, 1024, 128), BF16),
            pltpu.VMEM((4, 1024, 128), BF16),
            pltpu.VMEM((4, 1024, 128), BF16),
            pltpu.VMEM((1024, 128), BF16),
            pltpu.VMEM((2, 1024, 128), BF16),
            pltpu.VMEM((2, 1024, 128), BF16),
            pltpu.VMEM((16, NODES, HD), BF16),
            pltpu.VMEM((8, 2, NODES, HD), BF16),
            pltpu.VMEM((128, 1024), BF16),
            sems((6,)),
            sems((2, 4, 2)), sems((2, 4, 2)),
            sems((6,)), sems((6,)),
            sems((groups,)), sems((groups,)),
            sems((groups, 2)), sems((groups, 2)),
            sems((groups, 2)), sems((groups, 2)),
            sems((2, 8)), sems((2, 8)),
            sems((7,)), sems((7,)),
            sems((6,)), sems((6,)),
        ],
        compiler_params=pltpu.CompilerParams(
            collective_id=0, has_side_effects=True, vmem_limit_bytes=60000 * 1024
        ),
        name="verify",
    )(cache_lens, ints, queries, tree_keys, tree_values, cache_keys, cache_values, residual, out_weight)
    return hidden, accepted.reshape(512, 1024)


def solution(mesh):
    placed = (
        P("dp", "mp"),
        P("dp", "mp"),
        P("dp", "mp"),
        P("dp", None, "mp"),
        P("dp", None, "mp"),
        P("dp"),
        P("dp", None),
        P("dp", None),
        P("dp", "mp"),
        P("mp", "dp"),
    )
    return jax.shard_map(
        per_device,
        mesh=mesh,
        in_specs=placed,
        out_specs=(P("dp", "mp"), P(None, "mp")),
        check_vma=False,
    )
```

```python
import functools
import math

import jax
import jax.numpy as jnp
from jax import lax
from jax.experimental import pallas as pl
from jax.experimental.pallas import tpu as pltpu
from jax.sharding import PartitionSpec as P

F32, BF16 = jnp.float32, jnp.bfloat16
MESH = pl.DeviceIdType.MESH
Z, Y, X = 8, 4, 4
NODES, HD, GROUP = 64, 128, 8
SCALE = math.log2(math.e) / math.sqrt(HD)
NEG = -1e30
NT = (((1,), (1,)), ((), ()))
TN = (((0,), (0,)), ((), ()))
CHUNK = 2048
ROWS = 256
CACHE = 4096
OFFSET = (0, -1, 1, -2, 2, -3, 3, 4)
GROUPS = ((0, 0, 4), (1, 0, 4), (0, 4, 4), (1, 4, 4))
EXTRA = len(GROUPS)
TOTAL = 1024 + 128
UPWARD = (0, 1, 3, 5)


def kernel(
    lens_hbm, par_hbm, acn_hbm, q_hbm, tk_hbm, tv_hbm, k_hbm, v_hbm, res_hbm, w_hbm,
    hid_out, acc_out,
    lens, par, acn, q, tk, tv, kb, vb, m_s, l_s, acc_s, a_buf, e_buf, b_buf, part, pair_in, pair, r1_in, r2_src,
    r2_in, red, e_red, fin, e_fin, res,
    loc_sem, a_send, a_recv, e_send, e_recv, b_send, b_recv, d_send, d_recv, r1_send, r1_recv, r2_send, r2_recv,
    t_send, t_recv, et_send, et_recv, cz_send, cz_recv, cy_send, cy_recv,
):
    dp, m = lax.axis_index("dp"), lax.axis_index("mp")
    z, y = dp // Y, dp % Y
    x, c = m // 2, m % 2
    is_self = m == z

    def at_z(dz):
        return (((z + dz + Z) % Z) * Y + y, m)

    def at_y(dy):
        return (z * Y + (y + dy + Y) % Y, m)

    def at_x(dx):
        return (dp, ((x + dx + X) % X) * 2 + c)

    partner = (dp, x * 2 + (1 - c))

    barrier = pltpu.get_barrier_semaphore()

    def greet(peer):
        pl.semaphore_signal(barrier, inc=1, device_id=peer, device_id_type=MESH)

    for peer in [at_y(1), at_y(-1), at_z(1), at_z(-1), partner, at_x(1), at_x(-1)]:
        greet(peer)
    for other in range(8):

        @pl.when(jnp.logical_or(m != z, m != other))
        def _():
            greet((m * Y + y, other))

    local = {}
    for i, (name, src, dst) in enumerate(
        [("q", q_hbm, q), ("k0", k_hbm.at[0], kb.at[0]), ("v0", v_hbm.at[0], vb.at[0]), ("lens", lens_hbm, lens),
         ("par", par_hbm, par), ("acn", acn_hbm, acn), ("tk", tk_hbm, tk), ("tv", tv_hbm, tv),
         ("w", w_hbm, b_buf.at[0]), ("k1", k_hbm.at[1], kb.at[1]), ("v1", v_hbm.at[1], vb.at[1]),
         ("res", res_hbm, res)]
    ):
        local[name] = pltpu.make_async_copy(src, dst, loc_sem.at[i])
        local[name].start()

    def remote(src, dst, send, recv, peer):
        return pltpu.make_async_remote_copy(
            src_ref=src, dst_ref=dst, send_sem=send, recv_sem=recv, device_id=peer, device_id_type=MESH
        )

    def ancestors():
        sub = lax.broadcasted_iota(jnp.int32, (NODES, NODES), 0)
        lane = lax.broadcasted_iota(jnp.int32, (NODES, NODES), 1)
        eye = jnp.where(sub == lane, 1.0, 0.0)
        reach = [jnp.where(sub == par[r:r + 1, :], 1.0, 0.0) + eye for r in range(2)]
        for _ in range(6):
            step = [one.astype(BF16) for one in reach]
            reach = [jnp.minimum(jnp.dot(one, one, preferred_element_type=F32), 1.0) for one in step]
        sub = lax.broadcasted_iota(jnp.int32, (NODES, 128), 0)
        lane = lax.broadcasted_iota(jnp.int32, (NODES, 128), 1)
        return [
            lax.dot_general(
                reach[r].astype(BF16), jnp.where(sub + r * NODES == lane, 1.0, 0.0).astype(BF16), TN,
                preferred_element_type=F32,
            )
            for r in range(2)
        ]

    def picked(r, rows):
        nodes = lax.broadcasted_iota(jnp.int32, (NODES, 8), 0)
        pick = jnp.where(nodes == acn[r:r + 1, :], 1.0, 0.0).astype(BF16)
        return lax.dot_general(pick, rows, TN, preferred_element_type=F32)

    heads = ROWS // NODES

    def query_rows(r, b):
        return jnp.concatenate(
            [q[r * NODES:(r + 1) * NODES, h * HD:(h + 1) * HD] for h in range(b * heads, (b + 1) * heads)], axis=0
        )

    def absorb(r, j):
        count = lens[r]
        base = j * CHUNK
        keys = kb[r, base:base + CHUNK, :]
        values = vb[r, base:base + CHUNK, :]
        first = j == 0
        live = (lax.broadcasted_iota(jnp.int32, (1, CHUNK), 1) + base) < count
        bias = jnp.where(live, 0.0, NEG)
        for b in range(512 // ROWS):
            rows = slice(b * ROWS, (b + 1) * ROWS)
            s = lax.dot_general(query_rows(r, b), keys, NT, preferred_element_type=F32) * SCALE
            cols = [slice(t * 128, (t + 1) * 128) for t in range(CHUNK // 128)]
            scores = [s[:, t] if base + t.stop <= 1024 else s[:, t] + bias[:, t] for t in cols]
            top = functools.reduce(jnp.maximum, scores)
            new = jnp.broadcast_to(jnp.max(top, axis=1, keepdims=True), (ROWS, 128))
            if not first:
                old = m_s[rows, :]
                new = jnp.maximum(old, new)
                rescale = jnp.exp2(old - new)
            m_s[rows, :] = new
            weights = [jnp.exp2(one - new) for one in scores]
            total = functools.reduce(jnp.add, weights)
            out = jnp.dot(
                jnp.concatenate([one.astype(BF16) for one in weights], axis=1), values, preferred_element_type=F32
            )
            l_s[rows, :] = total if first else l_s[rows, :] * rescale + total
            acc_s[rows, :] = out if first else acc_s[rows, :] * rescale + out

    def close(r, reach):
        mask = jnp.concatenate([reach[r] > 0.5] * heads, axis=0)
        for b in range(512 // ROWS):
            rows = slice(b * ROWS, (b + 1) * ROWS)
            s = lax.dot_general(query_rows(r, b), tk[...], NT, preferred_element_type=F32) * SCALE
            s = jnp.where(mask, s, NEG)
            old = m_s[rows, :]
            new = jnp.maximum(old, jnp.broadcast_to(jnp.max(s, axis=1, keepdims=True), (ROWS, 128)))
            rescale = jnp.exp2(old - new)
            p = jnp.exp2(s - new)
            total = jnp.sum(l_s[rows, :] * rescale + p, axis=1, keepdims=True)
            out = acc_s[rows, :] * rescale + jnp.dot(p.astype(BF16), tv[...], preferred_element_type=F32)
            out = (out / total).astype(BF16)
            for h in range(heads):
                col = (b * heads + h) * HD
                a_buf[r, 0, :, col:col + HD] = out[h * NODES:(h + 1) * NODES, :]

    def a_copy(r, s, way):
        sign = 1 if way == 0 else -1
        src = 0 if s == 1 else 2 * (s - 1) - 1 + way
        if s < 4:
            dst, cut = 2 * s - 1 + way, slice(None)
        else:
            dst, cut = 7, slice(32 * way, 32 * way + 32)
        return remote(
            a_buf.at[r, src, cut], a_buf.at[r, dst, cut], a_send.at[r, s - 1, way], a_recv.at[r, s - 1, way], at_z(sign)
        )

    def a_go(r, s):
        for way in range(2):
            if s > 1:
                a_copy(r, s - 1, way).wait_recv()
            a_copy(r, s, way).start()

    def a_end(r):
        for way in range(2):
            a_copy(r, 4, way).wait_recv()

    def e_copy(s, way):
        sign = 1 if way == 0 else -1
        src = 0 if s == 1 else 2 * (s - 1) - 1 + way
        if s < 4:
            dst, cut = 2 * s - 1 + way, slice(None)
        else:
            dst, cut = 7, slice(512 * way, 512 * way + 512)
        return remote(
            e_buf.at[src, :, cut], e_buf.at[dst, :, cut], e_send.at[s - 1, way], e_recv.at[s - 1, way], at_z(sign)
        )

    def e_go(s):
        for way in range(2):
            if s > 1:
                e_copy(s - 1, way).wait_recv()
            e_copy(s, way).start()

    def e_end():
        for way in range(2):
            e_copy(4, way).wait_recv()

    def e_pick():
        rows = [picked(r, a_buf[r, 0]) for r in range(2)]
        e_buf[0] = jnp.concatenate(rows, axis=0).astype(BF16)

    def y_copies(view, send, recv):
        up, down = at_y(1), at_y(-1)
        plan = [(0, 3, 0, up), (0, 1, 1, down), (0, 3, 1, up), (0, 1, 0, down), (3, 2, 0, up), (1, 2, 1, down)]
        return [
            remote(view(src, half), view(dst, half), send.at[i], recv.at[i], peer)
            for i, (src, dst, half, peer) in enumerate(plan)
        ]

    b_copies = y_copies(lambda slot, half: b_buf.at[slot, half * 512:(half + 1) * 512], b_send, b_recv)

    def forward(copies):
        for i in range(2):
            copies[i].wait_recv()
            copies[4 + i].start()

    def span(g):
        if g == EXTRA:
            return 1024, 128
        r, p0, n = GROUPS[g]
        return (r * 8 + p0) * NODES, n * NODES

    def multiply(g):
        start, size = span(g)
        if g == EXTRA:
            left = e_buf[...].reshape(size, 1024)
        else:
            r, p0, n = GROUPS[g]
            left = a_buf[r, p0:p0 + n].reshape(size, 1024)
        for rel in range(Y):
            product = jnp.dot(left, b_buf[rel], preferred_element_type=F32).astype(BF16)
            part[2 * rel, start:start + size, :] = product[:, :128]
            part[2 * rel + 1, start:start + size, :] = product[:, 128:]
        pair_copy(g).start()

    def pair_copy(g):
        start, size = span(g)
        return remote(
            part.at[pl.ds((1 - c) * 4, 4), start:start + size], pair_in.at[:, start:start + size],
            d_send.at[g], d_recv.at[g], partner,
        )

    def r1_copy(g, way):
        start, size = span(g)
        half = slice(start + way * size // 2, start + (way + 1) * size // 2)
        return remote(
            pair.at[(x + 2) % X, half], r1_in.at[half], r1_send.at[g, way], r1_recv.at[g, way], at_x(1 - 2 * way)
        )

    def add_pair(g):
        start, size = span(g)
        rows = slice(start, start + size)
        pair_copy(g).wait_recv()
        for i in range(X):
            pair[i, rows, :] = (part[c * 4 + i, rows, :].astype(F32) + pair_in[i, rows, :].astype(F32)).astype(BF16)
        for way in range(2):
            r1_copy(g, way).start()

    def r2_copy(g, way):
        start, size = span(g)
        rows = slice(start, start + size)
        return remote(
            r2_src.at[way, rows], r2_in.at[way, rows], r2_send.at[g, way], r2_recv.at[g, way], at_x(1 - 2 * way)
        )

    def add_far(g):
        start, size = span(g)
        for way in range(2):
            r1_copy(g, way).wait_recv()
            near = (x + 1 - 2 * way + X) % X
            for half in range(2):
                rows = slice(start + half * size // 2, start + (half + 1) * size // 2)
                value = pair[near, rows, :]
                if half == way:
                    value = (value.astype(F32) + r1_in[rows, :].astype(F32)).astype(BF16)
                r2_src[way, rows, :] = value
            r2_copy(g, way).start()

    part_of = c * 4 + x
    own_slice = ((y + part_of // 2) % Y) * 2 + part_of % 2

    def t_copy(r, p):
        return remote(
            red.at[r * 8 + p], fin.at[own_slice, r], t_send.at[r, p], t_recv.at[r, own_slice],
            (((z + OFFSET[p] + Z) % Z) * Y + y, z),
        )

    def et_copy(p):
        return remote(
            e_red.at[p], e_fin.at[own_slice], et_send.at[p], et_recv.at[own_slice],
            (((z + OFFSET[p] + Z) % Z) * Y + y, z),
        )

    def deliver(copy, p, keep):
        if p == 0:
            pl.when(jnp.logical_not(is_self))(lambda: copy(p).start())
            pl.when(is_self)(keep)
        else:
            copy(p).start()

    def spread(g):
        start, size = span(g)
        rows = slice(start, start + size)
        for way in range(2):
            r2_copy(g, way).wait_recv()
        total = pair[x, rows, :].astype(F32) + r2_in[0, rows, :].astype(F32) + r2_in[1, rows, :].astype(F32)
        total = total.astype(BF16)
        if g == EXTRA:
            e_red[...] = total.reshape(8, 16, HD)

            def keep():
                e_fin[own_slice] = e_red[0]

            for p in range(8):
                deliver(et_copy, p, keep)
            return
        r, p0, n = GROUPS[g]
        red[r * 8 + p0:r * 8 + p0 + n] = total.reshape(n, NODES, HD)

        def keep():
            fin[own_slice, r] = red[r * 8]

        for p in range(p0, p0 + n):
            deliver(functools.partial(t_copy, r), p, keep)

    def arrived(i):
        return jnp.logical_or(m != z, own_slice != i)

    def finish(r):
        rows = slice(r * NODES, (r + 1) * NODES)
        for i in range(8):

            @pl.when(arrived(i))
            def _():
                remote(red.at[0], fin.at[i, r], t_send.at[r, 0], t_recv.at[r, i], partner).wait_recv()

            cols = slice(i * HD, (i + 1) * HD)
            hid_out[rows, cols] = (res[rows, cols].astype(F32) + fin[i, r].astype(F32)).astype(BF16)

    def cz_copy(s, way):
        sign = 1 if way == 0 else -1
        block = acc_out.at[(z - sign * (s - 1) + Z) % Z, y]
        if s == 4:
            block = block.at[:, 512 * way:512 * way + 512]
        return remote(block, block, cz_send.at[s - 1, way], cz_recv.at[s - 1, way], at_z(sign))

    def cy_copy(p, i):
        dy = (0, 0, -1 if p in UPWARD else 1)[i]
        peer = at_y((1, -1, 1 if p in UPWARD else -1)[i])
        block = acc_out.at[(z + OFFSET[p] + Z) % Z, (y + dy + Y) % Y]
        return remote(block, block, cy_send.at[p, i], cy_recv.at[p, i], peer)

    def c_start():
        rows = [picked(r, res[r * NODES:(r + 1) * NODES, :]) for r in range(2)]
        rows = jnp.concatenate(rows, axis=0)
        for i in range(8):

            @pl.when(arrived(i))
            def _():
                remote(e_red.at[0], e_fin.at[i], et_send.at[0], et_recv.at[i], partner).wait_recv()

            cols = slice(i * HD, (i + 1) * HD)
            acc_out[z, y, :, cols] = (rows[:, cols] + e_fin[i].astype(F32)).astype(BF16)
        for way in range(2):
            cz_copy(1, way).start()
        c_out(0)

    def c_out(p):
        for i in range(2):
            cy_copy(p, i).start()

    def c_pass(p):
        cy_copy(p, 0 if p in UPWARD else 1).wait_recv()
        cy_copy(p, 2).start()

    def c_go(s):
        for way in range(2):
            cz_copy(s, way).wait_recv()
            if s < 4:
                cz_copy(s + 1, way).start()
        if s < 4:
            c_out(2 * s - 1)
            c_out(2 * s)
        else:
            c_out(7)

    def c_relay(s):
        for p in (0,) if s == 0 else (7,) if s == 4 else (2 * s - 1, 2 * s):
            c_pass(p)

    def c_end():
        for p in range(8):
            cy_copy(p, 1 if p in UPWARD else 0).wait_recv()
            cy_copy(p, 2).wait_recv()

    local["q"].wait()
    local["k0"].wait()
    local["lens"].wait()
    local["v0"].wait()
    absorb(0, 0)
    pl.semaphore_wait(barrier, jnp.where(is_self, 14, 15))
    local["w"].wait()
    for i in range(4):
        b_copies[i].start()
    absorb(0, 1)
    for name in ("par", "acn", "tk", "tv", "k1", "v1", "res"):
        local[name].wait()
    reach = ancestors()
    close(0, reach)
    a_go(0, 1)
    absorb(1, 0)
    absorb(1, 1)
    close(1, reach)
    e_pick()
    e_go(1)
    a_go(1, 1)
    e_go(2)
    a_go(0, 2)
    forward(b_copies)
    e_go(3)
    a_go(1, 2)
    e_go(4)
    a_go(0, 3)
    for i in (2, 3, 4, 5):
        b_copies[i].wait_recv()
    e_end()
    multiply(EXTRA)
    a_go(1, 3)
    multiply(0)
    add_pair(EXTRA)
    multiply(1)
    add_far(EXTRA)
    add_pair(0)
    a_go(0, 4)
    add_pair(1)
    spread(EXTRA)
    a_go(1, 4)
    add_far(0)
    add_far(1)
    a_end(0)
    multiply(2)
    spread(0)
    spread(1)
    c_start()
    a_end(1)
    multiply(3)
    add_pair(2)
    c_go(1)
    add_pair(3)
    c_relay(0)
    add_far(2)
    c_go(2)
    c_relay(1)
    add_far(3)
    c_go(3)
    c_relay(2)
    spread(2)
    c_go(4)
    c_relay(3)
    spread(3)
    c_relay(4)
    finish(0)
    finish(1)
    c_end()

    for r in range(2):
        for s in range(1, 5):
            for way in range(2):
                a_copy(r, s, way).wait_send()
    for s in range(1, 5):
        for way in range(2):
            e_copy(s, way).wait_send()
            cz_copy(s, way).wait_send()
    for p in range(8):
        for copy in (functools.partial(t_copy, 0), functools.partial(t_copy, 1), et_copy):
            if p == 0:
                pl.when(jnp.logical_not(is_self))(lambda copy=copy: copy(0).wait_send())
            else:
                copy(p).wait_send()
        for i in range(3):
            cy_copy(p, i).wait_send()
    for g in range(len(GROUPS) + 1):
        pair_copy(g).wait_send()
        for way in range(2):
            r1_copy(g, way).wait_send()
            r2_copy(g, way).wait_send()
    for copy in b_copies:
        copy.wait_send()


def per_device(
    queries, tree_keys, tree_values, cache_keys, cache_values, cache_lens, parents, accepted_nodes, residual, out_weight
):
    vmem = pl.BlockSpec(memory_space=pltpu.VMEM)
    hbm = pl.BlockSpec(memory_space=pl.ANY)
    sems = pltpu.SemaphoreType.DMA
    groups = len(GROUPS) + 1
    hidden, accepted = pl.pallas_call(
        kernel,
        out_shape=(
            jax.ShapeDtypeStruct((128, 1024), BF16),
            jax.ShapeDtypeStruct((Z, Y, 16, 1024), BF16),
        ),
        in_specs=[hbm] * 10,
        out_specs=(vmem, vmem),
        scratch_shapes=[
            pltpu.SMEM((2,), jnp.int32),
            pltpu.VMEM((2, NODES), jnp.int32),
            pltpu.VMEM((2, 8), jnp.int32),
            pltpu.VMEM((128, 1024), BF16),
            pltpu.VMEM((128, HD), BF16),
            pltpu.VMEM((128, HD), BF16),
            pltpu.VMEM((2, CACHE, HD), BF16),
            pltpu.VMEM((2, CACHE, HD), BF16),
            pltpu.VMEM((512, 128), F32),
            pltpu.VMEM((512, 128), F32),
            pltpu.VMEM((512, 128), F32),
            pltpu.VMEM((2, 8, NODES, 1024), BF16),
            pltpu.VMEM((8, 16, 1024), BF16),
            pltpu.VMEM((Y, 1024, 256), BF16),
            pltpu.VMEM((8, TOTAL, 128), BF16),
            pltpu.VMEM((4, TOTAL, 128), BF16),
            pltpu.VMEM((4, TOTAL, 128), BF16),
            pltpu.VMEM((TOTAL, 128), BF16),
            pltpu.VMEM((2, TOTAL, 128), BF16),
            pltpu.VMEM((2, TOTAL, 128), BF16),
            pltpu.VMEM((16, NODES, HD), BF16),
            pltpu.VMEM((8, 16, HD), BF16),
            pltpu.VMEM((8, 2, NODES, HD), BF16),
            pltpu.VMEM((8, 16, HD), BF16),
            pltpu.VMEM((128, 1024), BF16),
            sems((12,)),
            sems((2, 4, 2)), sems((2, 4, 2)),
            sems((4, 2)), sems((4, 2)),
            sems((6,)), sems((6,)),
            sems((groups,)), sems((groups,)),
            sems((groups, 2)), sems((groups, 2)),
            sems((groups, 2)), sems((groups, 2)),
            sems((2, 8)), sems((2, 8)),
            sems((8,)), sems((8,)),
            sems((4, 2)), sems((4, 2)),
            sems((8, 3)), sems((8, 3)),
        ],
        compiler_params=pltpu.CompilerParams(
            collective_id=0, has_side_effects=True, vmem_limit_bytes=60000 * 1024
        ),
        name="verify",
    )(
        cache_lens, parents, accepted_nodes, queries, tree_keys, tree_values, cache_keys, cache_values, residual,
        out_weight,
    )
    return hidden, accepted.reshape(512, 1024)


def solution(mesh):
    placed = (
        P("dp", "mp"),
        P("dp", "mp"),
        P("dp", "mp"),
        P("dp", None, "mp"),
        P("dp", None, "mp"),
        P("dp"),
        P("dp", None),
        P("dp", None),
        P("dp", "mp"),
        P("mp", "dp"),
    )
    return jax.shard_map(
        per_device,
        mesh=mesh,
        in_specs=placed,
        out_specs=(P("dp", "mp"), P(None, "mp")),
        check_vma=False,
    )
```

```python
import functools
import math

import jax
import jax.numpy as jnp
from jax import lax
from jax.experimental import pallas as pl
from jax.experimental.pallas import tpu as pltpu
from jax.sharding import PartitionSpec as P

F32, BF16 = jnp.float32, jnp.bfloat16
MESH = pl.DeviceIdType.MESH
Z, Y, X = 8, 4, 4
NODES, HD, GROUP = 64, 128, 8
SCALE = math.log2(math.e) / math.sqrt(HD)
NEG = -1e30
NT = (((1,), (1,)), ((), ()))
TN = (((0,), (0,)), ((), ()))
CHUNK = 2048
ROWS = 256
CACHE = 4096
OFFSET = (0, -1, 1, -2, 2, -3, 3, 4)
GROUPS = ((0, 0, 4), (1, 0, 4), (0, 4, 4), (1, 4, 4))
EXTRA = len(GROUPS)
PARTS = ((0, 3), (3, 5), (5, 7))


def kernel(
    lens_hbm, par_hbm, acn_hbm, q_hbm, tk_hbm, tv_hbm, k_hbm, v_hbm, res_hbm, w_hbm,
    hid_out, acc_out,
    lens, par, acn, q, tk, tv, kb, vb, m_s, l_s, acc_s, a_buf, e_buf, b_buf, part, pair_in, pair, r1_in, r2_src, r2_in, red, fin,
    rows_e, c_buf, res,
    loc_sem, a_send, a_recv, e_send, e_recv, b_send, b_recv, d_send, d_recv, r1_send, r1_recv, r2_send, r2_recv,
    t_send, t_recv, et_send, et_recv, cz_send, cz_recv, cy_send, cy_recv,
    cd_send, cd_recv,
):
    dp, m = lax.axis_index("dp"), lax.axis_index("mp")
    z, y = dp // Y, dp % Y
    x, c = m // 2, m % 2
    is_self = m == z

    def at_z(dz):
        return (((z + dz + Z) % Z) * Y + y, m)

    def at_y(dy):
        return (z * Y + (y + dy + Y) % Y, m)

    def at_x(dx):
        return (dp, ((x + dx + X) % X) * 2 + c)

    partner = (dp, x * 2 + (1 - c))

    barrier = pltpu.get_barrier_semaphore()

    def greet(peer):
        pl.semaphore_signal(barrier, inc=1, device_id=peer, device_id_type=MESH)

    for peer in [at_y(1), at_y(-1), at_z(1), at_z(-1), partner, at_x(1), at_x(-1)]:
        greet(peer)
    local = {}
    for i, (name, src, dst) in enumerate(
        [("par", par_hbm, par), ("acn", acn_hbm, acn), ("lens", lens_hbm, lens), ("w", w_hbm, b_buf.at[0]),
         ("q", q_hbm, q), ("tk", tk_hbm, tk), ("tv", tv_hbm, tv), ("k0", k_hbm.at[0], kb.at[0]),
         ("k1", k_hbm.at[1], kb.at[1]), ("v0", v_hbm.at[0], vb.at[0]), ("v1", v_hbm.at[1], vb.at[1]),
         ("res", res_hbm, res)]
    ):
        local[name] = pltpu.make_async_copy(src, dst, loc_sem.at[i])
        local[name].start()

    def remote(src, dst, send, recv, peer):
        return pltpu.make_async_remote_copy(
            src_ref=src, dst_ref=dst, send_sem=send, recv_sem=recv, device_id=peer, device_id_type=MESH
        )

    def ancestors():
        sub = lax.broadcasted_iota(jnp.int32, (NODES, NODES), 0)
        lane = lax.broadcasted_iota(jnp.int32, (NODES, NODES), 1)
        eye = jnp.where(sub == lane, 1.0, 0.0)
        reach = [jnp.where(sub == par[r:r + 1, :], 1.0, 0.0) + eye for r in range(2)]
        for _ in range(6):
            step = [one.astype(BF16) for one in reach]
            reach = [jnp.minimum(jnp.dot(one, one, preferred_element_type=F32), 1.0) for one in step]
        sub = lax.broadcasted_iota(jnp.int32, (NODES, 128), 0)
        lane = lax.broadcasted_iota(jnp.int32, (NODES, 128), 1)
        return [
            lax.dot_general(
                reach[r].astype(BF16), jnp.where(sub + r * NODES == lane, 1.0, 0.0).astype(BF16), TN,
                preferred_element_type=F32,
            )
            for r in range(2)
        ]

    def picked(r, rows):
        nodes = lax.broadcasted_iota(jnp.int32, (NODES, 8), 0)
        pick = jnp.where(nodes == acn[r:r + 1, :], 1.0, 0.0).astype(BF16)
        return lax.dot_general(pick, rows, TN, preferred_element_type=F32)

    heads = ROWS // NODES

    def query_rows(r, b):
        return jnp.concatenate(
            [q[r * NODES:(r + 1) * NODES, h * HD:(h + 1) * HD] for h in range(b * heads, (b + 1) * heads)], axis=0
        )

    def absorb(r, j):
        count = lens[r]
        base = j * CHUNK
        keys = kb[r, base:base + CHUNK, :]
        values = vb[r, base:base + CHUNK, :]
        first = j == 0
        live = (lax.broadcasted_iota(jnp.int32, (1, CHUNK), 1) + base) < count
        bias = jnp.where(live, 0.0, NEG)
        for b in range(512 // ROWS):
            rows = slice(b * ROWS, (b + 1) * ROWS)
            s = lax.dot_general(query_rows(r, b), keys, NT, preferred_element_type=F32) * SCALE
            cols = [slice(t * 128, (t + 1) * 128) for t in range(CHUNK // 128)]
            scores = [s[:, t] if base + t.stop <= 1024 else s[:, t] + bias[:, t] for t in cols]
            top = functools.reduce(jnp.maximum, scores)
            new = jnp.broadcast_to(jnp.max(top, axis=1, keepdims=True), (ROWS, 128))
            if not first:
                old = m_s[rows, :]
                new = jnp.maximum(old, new)
                rescale = jnp.exp2(old - new)
            m_s[rows, :] = new
            weights = [jnp.exp2(one - new) for one in scores]
            total = functools.reduce(jnp.add, weights)
            out = jnp.dot(
                jnp.concatenate([one.astype(BF16) for one in weights], axis=1), values, preferred_element_type=F32
            )
            l_s[rows, :] = total if first else l_s[rows, :] * rescale + total
            acc_s[rows, :] = out if first else acc_s[rows, :] * rescale + out

    def close(r, reach):
        mask = jnp.concatenate([reach[r] > 0.5] * heads, axis=0)
        for b in range(512 // ROWS):
            rows = slice(b * ROWS, (b + 1) * ROWS)
            s = lax.dot_general(query_rows(r, b), tk[...], NT, preferred_element_type=F32) * SCALE
            s = jnp.where(mask, s, NEG)
            old = m_s[rows, :]
            new = jnp.maximum(old, jnp.broadcast_to(jnp.max(s, axis=1, keepdims=True), (ROWS, 128)))
            rescale = jnp.exp2(old - new)
            p = jnp.exp2(s - new)
            total = jnp.sum(l_s[rows, :] * rescale + p, axis=1, keepdims=True)
            out = acc_s[rows, :] * rescale + jnp.dot(p.astype(BF16), tv[...], preferred_element_type=F32)
            out = (out / total).astype(BF16)
            for h in range(heads):
                col = (b * heads + h) * HD
                a_buf[r, 0, :, col:col + HD] = out[h * NODES:(h + 1) * NODES, :]

    def a_copy(r, s, way):
        sign = 1 if way == 0 else -1
        src = 0 if s == 1 else 2 * (s - 1) - 1 + way
        if s < 4:
            dst, cut = 2 * s - 1 + way, slice(None)
        else:
            dst, cut = 7, slice(32 * way, 32 * way + 32)
        return remote(
            a_buf.at[r, src, cut], a_buf.at[r, dst, cut], a_send.at[r, s - 1, way], a_recv.at[r, s - 1, way], at_z(sign)
        )

    def a_go(r, s):
        for way in range(2):
            if s > 1:
                a_copy(r, s - 1, way).wait_recv()
            a_copy(r, s, way).start()

    def a_end(r):
        for way in range(2):
            a_copy(r, 4, way).wait_recv()

    def e_copy(s, way):
        sign = 1 if way == 0 else -1
        src = 0 if s == 1 else 2 * (s - 1) - 1 + way
        if s < 4:
            dst, cut = 2 * s - 1 + way, slice(None)
        else:
            dst, cut = 7, slice(512 * way, 512 * way + 512)
        return remote(
            e_buf.at[src, :, cut], e_buf.at[dst, :, cut], e_send.at[s - 1, way], e_recv.at[s - 1, way], at_z(sign)
        )

    def e_go(s):
        for way in range(2):
            if s > 1:
                e_copy(s - 1, way).wait_recv()
            e_copy(s, way).start()

    def e_end():
        for way in range(2):
            e_copy(4, way).wait_recv()

    def e_attend(reach):
        outs = []
        for r in range(2):
            chosen = picked(r, q[r * NODES:(r + 1) * NODES, :])
            rows = jnp.concatenate([chosen[:, h * HD:(h + 1) * HD] for h in range(GROUP)], axis=0).astype(BF16)
            mask = jnp.concatenate([picked(r, reach[r].astype(BF16))] * GROUP, axis=0) > 0.5
            tree = lax.dot_general(rows, tk[...], NT, preferred_element_type=F32) * SCALE
            tree = jnp.where(mask, tree, NEG)
            s = lax.dot_general(rows, kb[r], NT, preferred_element_type=F32) * SCALE
            live = lax.broadcasted_iota(jnp.int32, (1, CACHE), 1) < lens[r]
            s = s + jnp.where(live, 0.0, NEG)
            cols = [s[:, t * 128:(t + 1) * 128] for t in range(CACHE // 128)]
            top = jnp.max(functools.reduce(jnp.maximum, cols + [tree]), axis=1, keepdims=True)
            weights = [jnp.exp2(one - top) for one in cols]
            first = jnp.exp2(tree - top)
            total = jnp.sum(functools.reduce(jnp.add, weights + [first]), axis=1, keepdims=True)
            out = jnp.dot(first.astype(BF16), tv[...], preferred_element_type=F32) + jnp.dot(
                jnp.concatenate([one.astype(BF16) for one in weights], axis=1), vb[r], preferred_element_type=F32
            )
            outs.append(out / total)
        for h in range(GROUP):
            block = jnp.concatenate([out[h * 8:(h + 1) * 8] for out in outs], axis=0)
            e_buf[0, :, h * HD:(h + 1) * HD] = block.astype(BF16)

    def y_copies(view, send, recv):
        up, down = at_y(1), at_y(-1)
        plan = [(0, 3, 0, up), (0, 1, 1, down), (0, 3, 1, up), (0, 1, 0, down), (3, 2, 0, up), (1, 2, 1, down)]
        return [
            remote(view(src, half), view(dst, half), send.at[i], recv.at[i], peer)
            for i, (src, dst, half, peer) in enumerate(plan)
        ]

    b_copies = y_copies(lambda slot, half: b_buf.at[slot, half * 512:(half + 1) * 512], b_send, b_recv)

    def forward(copies):
        for i in range(2):
            copies[i].wait_recv()
            copies[4 + i].start()

    def span(g):
        r, p0, n = GROUPS[g]
        return (r * 8 + p0) * NODES, n * NODES

    def multiply(g):
        start, size = span(g)
        r, p0, n = GROUPS[g]
        left = a_buf[r, p0:p0 + n].reshape(size, 1024)
        for rel in range(Y):
            product = jnp.dot(left, b_buf[rel], preferred_element_type=F32).astype(BF16)
            part[2 * rel, start:start + size, :] = product[:, :128]
            part[2 * rel + 1, start:start + size, :] = product[:, 128:]
        pair_copy(g).start()

    def pair_copy(g):
        start, size = span(g)
        return remote(
            part.at[pl.ds((1 - c) * 4, 4), start:start + size], pair_in.at[:, start:start + size],
            d_send.at[g], d_recv.at[g], partner,
        )

    def r1_copy(g, way):
        start, size = span(g)
        half = slice(start + way * size // 2, start + (way + 1) * size // 2)
        return remote(
            pair.at[(x + 2) % X, half], r1_in.at[half], r1_send.at[g, way], r1_recv.at[g, way], at_x(1 - 2 * way)
        )

    def add_pair(g):
        start, size = span(g)
        rows = slice(start, start + size)
        pair_copy(g).wait_recv()
        for i in range(X):
            pair[i, rows, :] = (part[c * 4 + i, rows, :].astype(F32) + pair_in[i, rows, :].astype(F32)).astype(BF16)
        for way in range(2):
            r1_copy(g, way).start()

    def r2_copy(g, way):
        start, size = span(g)
        rows = slice(start, start + size)
        return remote(
            r2_src.at[way, rows], r2_in.at[way, rows], r2_send.at[g, way], r2_recv.at[g, way], at_x(1 - 2 * way)
        )

    def add_far(g):
        start, size = span(g)
        for way in range(2):
            r1_copy(g, way).wait_recv()
            near = (x + 1 - 2 * way + X) % X
            for half in range(2):
                rows = slice(start + half * size // 2, start + (half + 1) * size // 2)
                value = pair[near, rows, :]
                if half == way:
                    value = (value.astype(F32) + r1_in[rows, :].astype(F32)).astype(BF16)
                r2_src[way, rows, :] = value
            r2_copy(g, way).start()

    part_of = c * 4 + x
    own_slice = ((y + part_of // 2) % Y) * 2 + part_of % 2

    def t_copy(r, p):
        return remote(
            red.at[r * 8 + p], fin.at[own_slice, r], t_send.at[r, p], t_recv.at[r, own_slice],
            (((z + OFFSET[p] + Z) % Z) * Y + y, z),
        )

    def deliver(copy, p, keep):
        if p == 0:
            pl.when(jnp.logical_not(is_self))(lambda: copy(p).start())
            pl.when(is_self)(keep)
        else:
            copy(p).start()

    def spread(g):
        start, size = span(g)
        rows = slice(start, start + size)
        for way in range(2):
            r2_copy(g, way).wait_recv()
        total = pair[x, rows, :].astype(F32) + r2_in[0, rows, :].astype(F32) + r2_in[1, rows, :].astype(F32)
        total = total.astype(BF16)
        r, p0, n = GROUPS[g]
        red[r * 8 + p0:r * 8 + p0 + n] = total.reshape(n, NODES, HD)

        def keep():
            fin[own_slice, r] = red[r * 8]

        for p in range(p0, p0 + n):
            deliver(functools.partial(t_copy, r), p, keep)

    def arrived(i):
        return jnp.logical_or(m != z, own_slice != i)

    def finish(r):
        rows = slice(r * NODES, (r + 1) * NODES)
        for i in range(8):

            @pl.when(arrived(i))
            def _():
                remote(red.at[0], fin.at[i, r], t_send.at[r, 0], t_recv.at[r, i], partner).wait_recv()

            cols = slice(i * HD, (i + 1) * HD)
            hid_out[rows, cols] = (res[rows, cols].astype(F32) + fin[i, r].astype(F32)).astype(BF16)


    def bufs(g):
        return rows_e, 0, 0, 8

    def e_multiply(g):
        (part, *_), r, n0, n1 = bufs(g)
        size = part.shape[-2]
        left = e_buf[...].reshape(8 * size, 1024)
        for rel in range(n0 // 2, n1 // 2):
            product = jnp.dot(left, b_buf[rel], preferred_element_type=F32).astype(BF16)
            for p in range(8):
                block = (z + OFFSET[p] + Z) % Z
                for half in range(2):
                    part[r, block // 2, block % 2, 2 * rel + half] = product[
                        p * size:(p + 1) * size, half * 128:half * 128 + 128
                    ]
        e_pair_copy(g).start()

    def e_pair_copy(g):
        (part, pair_in, *_), r, n0, n1 = bufs(g)
        return remote(
            part.at[r, :, 1 - c, n0:n1], pair_in.at[r, :, n0:n1], d_send.at[g], d_recv.at[g], partner
        )

    def e_r1_copy(g, way):
        (_, _, pair, r1_in, *_), r, n0, n1 = bufs(g)
        n = (n1 - n0) // 2
        half = slice(n0 + way * n, n0 + way * n + n)
        return remote(
            pair.at[r, (x + 2) % X, half], r1_in.at[r, half], r1_send.at[g, way], r1_recv.at[g, way],
            at_x(1 - 2 * way),
        )

    def e_add_pair(g):
        (part, pair_in, pair, *_), r, n0, n1 = bufs(g)
        e_pair_copy(g).wait_recv()
        for i in range(X):
            pair[r, i, n0:n1] = (part[r, i, c, n0:n1].astype(F32) + pair_in[r, i, n0:n1].astype(F32)).astype(BF16)
        for way in range(2):
            e_r1_copy(g, way).start()

    def e_r2_copy(g, way):
        (_, _, _, _, r2_src, r2_in, *_), r, n0, n1 = bufs(g)
        return remote(
            r2_src.at[way, r, n0:n1], r2_in.at[way, r, n0:n1], r2_send.at[g, way], r2_recv.at[g, way],
            at_x(1 - 2 * way),
        )

    def e_add_far(g):
        (_, _, pair, r1_in, r2_src, *_), r, n0, n1 = bufs(g)
        n = (n1 - n0) // 2
        for way in range(2):
            e_r1_copy(g, way).wait_recv()
            near = (x + 1 - 2 * way + X) % X
            for half in range(2):
                part_n = slice(n0 + half * n, n0 + half * n + n)
                value = pair[r, near, part_n]
                if half == way:
                    value = (value.astype(F32) + r1_in[r, part_n].astype(F32)).astype(BF16)
                r2_src[way, r, part_n] = value
            e_r2_copy(g, way).start()

    def e_t_copy(g):
        (*_, red, fin), r, n0, n1 = bufs(g)
        return remote(red.at[r, n0:n1], fin.at[r, n0:n1], et_send.at[0], et_recv.at[0], (m * Y + y, z))

    def e_spread(g):
        (_, _, pair, _, _, r2_in, red, fin), r, n0, n1 = bufs(g)
        for way in range(2):
            e_r2_copy(g, way).wait_recv()
        total = pair[r, x, n0:n1].astype(F32) + r2_in[0, r, n0:n1].astype(F32) + r2_in[1, r, n0:n1].astype(F32)
        red[r, n0:n1] = total.astype(BF16)
        pl.when(jnp.logical_not(is_self))(lambda: e_t_copy(g).start())

        @pl.when(is_self)
        def _():
            fin[r, n0:n1] = red[r, n0:n1]

    def e_t_wait(g):
        pl.when(jnp.logical_not(is_self))(lambda: e_t_copy(g).wait_recv())

    def e_summed(g, i):
        (*_, fin), r, _, _ = bufs(g)
        return fin[r, ((i // 2 - y + Y) % Y) * 2 + i % 2].astype(F32)

    def cz_copy(s, way):
        sign = 1 if way == 0 else -1
        src = 0 if s == 1 else 2 * (s - 1) - 1 + way
        dst = 2 * s - 1 + way
        return remote(
            c_buf.at[src, y], c_buf.at[dst, y], cz_send.at[s - 1, way], cz_recv.at[s - 1, way], at_z(sign)
        )

    def cd_copy(way, i, dy, from_y):
        sign = 1 if way == 0 else -1
        cut = slice(512 * way, 512 * way + 512)
        peer = (((z + sign + Z) % Z) * Y + (y + dy) % Y, m)
        return remote(
            c_buf.at[5 + way, from_y, :, cut], c_buf.at[7, from_y, :, cut], cd_send.at[way, i],
            cd_recv.at[way, from_y], peer,
        )

    def cy_copy(part, i):
        slots = slice(*PARTS[part])
        if i < 2:
            return remote(
                c_buf.at[slots, y], c_buf.at[slots, y], cy_send.at[part, i], cy_recv.at[part, i], at_y(1 - 2 * i)
            )
        way = i - 2
        src = (y - 1 + 2 * way + Y) % Y
        block = c_buf.at[slots, src, :, 512 * way:512 * way + 512]
        return remote(block, block, cy_send.at[part, i], cy_recv.at[part, i], at_y(1 - 2 * way))

    def c_start():
        rows = [picked(r, res[r * NODES:(r + 1) * NODES, :]) for r in range(2)]
        rows = jnp.concatenate(rows, axis=0)
        e_t_wait(EXTRA)
        for i in range(8):
            cols = slice(i * HD, (i + 1) * HD)
            c_buf[0, y, :, cols] = (rows[:, cols] + e_summed(EXTRA, i)).astype(BF16)
        for way in range(2):
            cz_copy(1, way).start()

    def c_go(s):
        for way in range(2):
            cz_copy(s, way).wait_recv()
            if s < 3:
                cz_copy(s + 1, way).start()
            else:
                for dy in range(Y):
                    cd_copy(way, dy, dy, y).start()
        for i in range(2):
            cy_copy(s - 1, i).start()

    def c_relay(part):
        for way in range(2):
            cy_copy(part, way).wait_recv()
            cy_copy(part, 2 + way).start()

    def c_end(part):
        for way in range(2):
            cy_copy(part, 2 + way).wait_recv()
        if part == 2:
            for way in range(2):
                for from_y in range(Y):
                    cd_copy(way, 0, 0, from_y).wait_recv()
            acc_out[(z + 4) % Z] = c_buf[7]
        for p in range(*PARTS[part]):
            acc_out[(z + OFFSET[p] + Z) % Z] = c_buf[p]

    local["par"].wait()
    local["acn"].wait()
    reach = ancestors()
    pl.semaphore_wait(barrier, 7)
    local["w"].wait()
    for i in range(4):
        b_copies[i].start()
    for name in ("lens", "q", "tk", "tv", "k0", "k1", "v0", "v1"):
        local[name].wait()
    e_attend(reach)
    e_go(1)
    absorb(0, 0)
    absorb(0, 1)
    e_go(2)
    close(0, reach)
    a_go(0, 1)
    absorb(1, 0)
    forward(b_copies)
    absorb(1, 1)
    e_go(3)
    close(1, reach)
    a_go(1, 1)
    e_go(4)
    a_go(0, 2)
    a_go(1, 2)
    e_end()
    a_go(0, 3)
    for i in (2, 3, 4, 5):
        b_copies[i].wait_recv()
    e_multiply(EXTRA)
    multiply(0)
    a_go(1, 3)
    e_add_pair(EXTRA)
    multiply(1)
    add_pair(0)
    a_go(0, 4)
    e_add_far(EXTRA)
    add_pair(1)
    a_go(1, 4)
    add_far(0)
    e_spread(EXTRA)
    add_far(1)
    a_end(0)
    multiply(2)
    a_end(1)
    multiply(3)
    spread(0)
    add_pair(2)
    local["res"].wait()
    c_start()
    spread(1)
    add_pair(3)
    c_go(1)
    add_far(2)
    add_far(3)
    c_go(2)
    c_go(3)
    spread(2)
    spread(3)
    c_relay(0)
    c_relay(1)
    c_end(0)
    c_relay(2)
    c_end(1)
    finish(0)
    finish(1)
    c_end(2)

    for s in range(1, 5):
        for way in range(2):
            a_copy(0, s, way).wait_send()
            a_copy(1, s, way).wait_send()
            e_copy(s, way).wait_send()
            if s < 4:
                cz_copy(s, way).wait_send()
            cd_copy(way, s - 1, s - 1, y).wait_send()
    for part_number in range(len(PARTS)):
        for i in range(4):
            cy_copy(part_number, i).wait_send()
    for g in range(len(GROUPS)):
        pair_copy(g).wait_send()
        for way in range(2):
            r1_copy(g, way).wait_send()
            r2_copy(g, way).wait_send()
    e_pair_copy(EXTRA).wait_send()
    for way in range(2):
        e_r1_copy(EXTRA, way).wait_send()
        e_r2_copy(EXTRA, way).wait_send()
    for r in range(2):
        pl.when(jnp.logical_not(is_self))(lambda r=r: t_copy(r, 0).wait_send())
        for p in range(1, 8):
            t_copy(r, p).wait_send()
    pl.when(jnp.logical_not(is_self))(lambda: e_t_copy(EXTRA).wait_send())
    for copy in b_copies:
        copy.wait_send()


def per_device(
    queries, tree_keys, tree_values, cache_keys, cache_values, cache_lens, parents, accepted_nodes, residual, out_weight
):
    vmem = pl.BlockSpec(memory_space=pltpu.VMEM)
    hbm = pl.BlockSpec(memory_space=pl.ANY)
    sems = pltpu.SemaphoreType.DMA
    groups = len(GROUPS) + 1

    def summing(count, size):
        shapes = [
            (count, X, 2, 8), (count, X, 8), (count, X, 8), (count, 8), (2, count, 8), (2, count, 8), (count, 8),
            (count, 8),
        ]
        return [pltpu.VMEM((*dims, size, HD), BF16) for dims in shapes]

    hidden, accepted = pl.pallas_call(
        kernel,
        out_shape=(
            pltpu.VMEM((128, 1024), BF16),
            pltpu.VMEM((Z, Y, 16, 1024), BF16),
        ),
        in_specs=[hbm] * 10,
        out_specs=(vmem, vmem),
        scratch_shapes=[
            pltpu.SMEM((2,), jnp.int32),
            pltpu.VMEM((2, NODES), jnp.int32),
            pltpu.VMEM((2, 8), jnp.int32),
            pltpu.VMEM((128, 1024), BF16),
            pltpu.VMEM((128, HD), BF16),
            pltpu.VMEM((128, HD), BF16),
            pltpu.VMEM((2, CACHE, HD), BF16),
            pltpu.VMEM((2, CACHE, HD), BF16),
            pltpu.VMEM((512, 128), F32),
            pltpu.VMEM((512, 128), F32),
            pltpu.VMEM((512, 128), F32),
            pltpu.VMEM((2, 8, NODES, 1024), BF16),
            pltpu.VMEM((8, 16, 1024), BF16),
            pltpu.VMEM((Y, 1024, 256), BF16),
            pltpu.VMEM((8, 1024, 128), BF16),
            pltpu.VMEM((4, 1024, 128), BF16),
            pltpu.VMEM((4, 1024, 128), BF16),
            pltpu.VMEM((1024, 128), BF16),
            pltpu.VMEM((2, 1024, 128), BF16),
            pltpu.VMEM((2, 1024, 128), BF16),
            pltpu.VMEM((16, NODES, HD), BF16),
            pltpu.VMEM((8, 2, NODES, HD), BF16),
            summing(1, 16),
            pltpu.VMEM((8, Y, 16, 1024), BF16),
            pltpu.VMEM((128, 1024), BF16),
            sems((12,)),
            sems((2, 4, 2)), sems((2, 4, 2)),
            sems((4, 2)), sems((4, 2)),
            sems((6,)), sems((6,)),
            sems((groups,)), sems((groups,)),
            sems((groups, 2)), sems((groups, 2)),
            sems((groups, 2)), sems((groups, 2)),
            sems((2, 8)), sems((2, 8)),
            sems((1,)), sems((1,)),
            sems((3, 2)), sems((3, 2)),
            sems((3, 4)), sems((3, 4)),
            sems((2, 4)), sems((2, 4)),
        ],
        compiler_params=pltpu.CompilerParams(
            collective_id=0, has_side_effects=True, vmem_limit_bytes=60000 * 1024
        ),
        name="verify",
    )(
        cache_lens, parents, accepted_nodes, queries, tree_keys, tree_values, cache_keys, cache_values, residual,
        out_weight,
    )
    return hidden, accepted.reshape(512, 1024)


def solution(mesh):
    placed = (
        P("dp", "mp"),
        P("dp", "mp"),
        P("dp", "mp"),
        P("dp", None, "mp"),
        P("dp", None, "mp"),
        P("dp"),
        P("dp", None),
        P("dp", None),
        P("dp", "mp"),
        P("mp", "dp"),
    )
    return jax.shard_map(
        per_device,
        mesh=mesh,
        in_specs=placed,
        out_specs=(P("dp", "mp"), P(None, "mp")),
        check_vma=False,
    )
```

```python
import functools
import math

import jax
import jax.numpy as jnp
from jax import lax
from jax.experimental import pallas as pl
from jax.experimental.pallas import tpu as pltpu
from jax.sharding import PartitionSpec as P

F32, BF16 = jnp.float32, jnp.bfloat16
MESH = pl.DeviceIdType.MESH
Z, Y, X = 8, 4, 4
NODES, HD, GROUP = 64, 128, 8
SCALE = math.log2(math.e) / math.sqrt(HD)
NEG = -1e30
NT = (((1,), (1,)), ((), ()))
TN = (((0,), (0,)), ((), ()))
CHUNK = 2048
ROWS = 256
CACHE = 4096
OFFSET = (0, -1, 1, -2, 2, -3, 3, 4)
GROUPS = ((0, 0, 4), (1, 0, 4), (0, 4, 4), (1, 4, 4))
EXTRA = len(GROUPS)
PARTS = ((0, 3), (3, 5), (5, 7))


def kernel(
    lens_hbm, par_hbm, acn_hbm, q_hbm, tk_hbm, tv_hbm, k_hbm, v_hbm, res_hbm, w_hbm,
    hid_out, acc_out,
    lens, par, acn, q, tk, tv, kb, vb, m_s, l_s, acc_s, a_buf, e_buf, b_buf, part, pair_in, pair, r1_in, r2_src, r2_in, red, fin,
    rows_e, c_buf, res,
    loc_sem, a_send, a_recv, e_send, e_recv, b_send, b_recv, d_send, d_recv, r1_send, r1_recv, r2_send, r2_recv,
    t_send, t_recv, et_send, et_recv, cz_send, cz_recv, cy_send, cy_recv,
    cd_send, cd_recv,
):
    dp, m = lax.axis_index("dp"), lax.axis_index("mp")
    z, y = dp // Y, dp % Y
    x, c = m // 2, m % 2
    is_self = m == z

    def at_z(dz):
        return (((z + dz + Z) % Z) * Y + y, m)

    def at_y(dy):
        return (z * Y + (y + dy + Y) % Y, m)

    def at_x(dx):
        return (dp, ((x + dx + X) % X) * 2 + c)

    partner = (dp, x * 2 + (1 - c))

    barrier = pltpu.get_barrier_semaphore()

    def greet(peer):
        pl.semaphore_signal(barrier, inc=1, device_id=peer, device_id_type=MESH)

    for peer in [at_y(1), at_y(-1), at_z(1), at_z(-1), partner, at_x(1), at_x(-1)]:
        greet(peer)
    local = {}
    for i, (name, src, dst) in enumerate(
        [("w", w_hbm, b_buf.at[0]), ("par", par_hbm, par), ("acn", acn_hbm, acn), ("lens", lens_hbm, lens),
         ("q", q_hbm, q), ("tk", tk_hbm, tk), ("tv", tv_hbm, tv), ("k0", k_hbm.at[0], kb.at[0]),
         ("k1", k_hbm.at[1], kb.at[1]), ("v0", v_hbm.at[0], vb.at[0]), ("v1", v_hbm.at[1], vb.at[1]),
         ("res", res_hbm, res)]
    ):
        local[name] = pltpu.make_async_copy(src, dst, loc_sem.at[i])
        local[name].start()

    def remote(src, dst, send, recv, peer):
        return pltpu.make_async_remote_copy(
            src_ref=src, dst_ref=dst, send_sem=send, recv_sem=recv, device_id=peer, device_id_type=MESH
        )

    def drained(view, sem):
        remote(view, view, sem, sem, partner).wait_send()

    def received(view, sem):
        remote(view, view, sem, sem, partner).wait_recv()

    def ancestors():
        sub = lax.broadcasted_iota(jnp.int32, (NODES, NODES), 0)
        lane = lax.broadcasted_iota(jnp.int32, (NODES, NODES), 1)
        eye = jnp.where(sub == lane, 1.0, 0.0)
        reach = [jnp.where(sub == par[r:r + 1, :], 1.0, 0.0) + eye for r in range(2)]
        for _ in range(6):
            step = [one.astype(BF16) for one in reach]
            reach = [jnp.minimum(jnp.dot(one, one, preferred_element_type=F32), 1.0) for one in step]
        sub = lax.broadcasted_iota(jnp.int32, (NODES, 128), 0)
        lane = lax.broadcasted_iota(jnp.int32, (NODES, 128), 1)
        return [
            lax.dot_general(
                reach[r].astype(BF16), jnp.where(sub + r * NODES == lane, 1.0, 0.0).astype(BF16), TN,
                preferred_element_type=F32,
            )
            for r in range(2)
        ]

    def picked(r, rows):
        nodes = lax.broadcasted_iota(jnp.int32, (NODES, 8), 0)
        pick = jnp.where(nodes == acn[r:r + 1, :], 1.0, 0.0).astype(BF16)
        return lax.dot_general(pick, rows, TN, preferred_element_type=F32)

    heads = ROWS // NODES

    def query_rows(r, b):
        return jnp.concatenate(
            [q[r * NODES:(r + 1) * NODES, h * HD:(h + 1) * HD] for h in range(b * heads, (b + 1) * heads)], axis=0
        )

    def absorb(r, j):
        count = lens[r]
        base = j * CHUNK
        keys = kb[r, base:base + CHUNK, :]
        values = vb[r, base:base + CHUNK, :]
        first = j == 0
        live = (lax.broadcasted_iota(jnp.int32, (1, CHUNK), 1) + base) < count
        bias = jnp.where(live, 0.0, NEG)
        for b in range(512 // ROWS):
            rows = slice(b * ROWS, (b + 1) * ROWS)
            s = lax.dot_general(query_rows(r, b), keys, NT, preferred_element_type=F32) * SCALE
            cols = [slice(t * 128, (t + 1) * 128) for t in range(CHUNK // 128)]
            scores = [s[:, t] if base + t.stop <= 1024 else s[:, t] + bias[:, t] for t in cols]
            top = functools.reduce(jnp.maximum, scores)
            new = jnp.broadcast_to(jnp.max(top, axis=1, keepdims=True), (ROWS, 128))
            if not first:
                old = m_s[rows, :]
                new = jnp.maximum(old, new)
                rescale = jnp.exp2(old - new)
            m_s[rows, :] = new
            weights = [jnp.exp2(one - new) for one in scores]
            total = functools.reduce(jnp.add, weights)
            out = jnp.dot(
                jnp.concatenate([one.astype(BF16) for one in weights], axis=1), values, preferred_element_type=F32
            )
            l_s[rows, :] = total if first else l_s[rows, :] * rescale + total
            acc_s[rows, :] = out if first else acc_s[rows, :] * rescale + out

    def close(r, reach):
        mask = jnp.concatenate([reach[r] > 0.5] * heads, axis=0)
        for b in range(512 // ROWS):
            rows = slice(b * ROWS, (b + 1) * ROWS)
            s = lax.dot_general(query_rows(r, b), tk[...], NT, preferred_element_type=F32) * SCALE
            s = jnp.where(mask, s, NEG)
            old = m_s[rows, :]
            new = jnp.maximum(old, jnp.broadcast_to(jnp.max(s, axis=1, keepdims=True), (ROWS, 128)))
            rescale = jnp.exp2(old - new)
            p = jnp.exp2(s - new)
            total = jnp.sum(l_s[rows, :] * rescale + p, axis=1, keepdims=True)
            out = acc_s[rows, :] * rescale + jnp.dot(p.astype(BF16), tv[...], preferred_element_type=F32)
            out = (out / total).astype(BF16)
            for h in range(heads):
                col = (b * heads + h) * HD
                a_buf[r, 0, :, col:col + HD] = out[h * NODES:(h + 1) * NODES, :]

    def a_copy(r, s, way):
        sign = 1 if way == 0 else -1
        src = 0 if s == 1 else 2 * (s - 1) - 1 + way
        if s < 4:
            dst, cut = 2 * s - 1 + way, slice(None)
        else:
            dst, cut = 7, slice(32 * way, 32 * way + 32)
        return remote(
            a_buf.at[r, src, cut], a_buf.at[r, dst, cut], a_send.at[0], a_recv.at[r, s - 1, way], at_z(sign)
        )

    def a_go(r, s):
        for way in range(2):
            if s > 1:
                a_copy(r, s - 1, way).wait_recv()
            a_copy(r, s, way).start()

    def a_end(r):
        for way in range(2):
            a_copy(r, 4, way).wait_recv()

    def e_copy(s, way):
        sign = 1 if way == 0 else -1
        src = 0 if s == 1 else 2 * (s - 1) - 1 + way
        if s < 4:
            dst, cut = 2 * s - 1 + way, slice(None)
        else:
            dst, cut = 7, slice(512 * way, 512 * way + 512)
        return remote(
            e_buf.at[src, :, cut], e_buf.at[dst, :, cut], e_send.at[0], e_recv.at[s - 1, way], at_z(sign)
        )

    def e_go(s):
        for way in range(2):
            if s > 1:
                e_copy(s - 1, way).wait_recv()
            e_copy(s, way).start()

    def e_end():
        for way in range(2):
            e_copy(4, way).wait_recv()

    def e_attend(reach):
        outs = []
        for r in range(2):
            chosen = picked(r, q[r * NODES:(r + 1) * NODES, :])
            rows = jnp.concatenate([chosen[:, h * HD:(h + 1) * HD] for h in range(GROUP)], axis=0).astype(BF16)
            mask = jnp.concatenate([picked(r, reach[r].astype(BF16))] * GROUP, axis=0) > 0.5
            tree = lax.dot_general(rows, tk[...], NT, preferred_element_type=F32) * SCALE
            tree = jnp.where(mask, tree, NEG)
            s = lax.dot_general(rows, kb[r], NT, preferred_element_type=F32) * SCALE
            live = lax.broadcasted_iota(jnp.int32, (1, CACHE), 1) < lens[r]
            s = s + jnp.where(live, 0.0, NEG)
            cols = [s[:, t * 128:(t + 1) * 128] for t in range(CACHE // 128)]
            top = jnp.max(functools.reduce(jnp.maximum, cols + [tree]), axis=1, keepdims=True)
            weights = [jnp.exp2(one - top) for one in cols]
            first = jnp.exp2(tree - top)
            total = jnp.sum(functools.reduce(jnp.add, weights + [first]), axis=1, keepdims=True)
            out = jnp.dot(first.astype(BF16), tv[...], preferred_element_type=F32) + jnp.dot(
                jnp.concatenate([one.astype(BF16) for one in weights], axis=1), vb[r], preferred_element_type=F32
            )
            outs.append(out / total)
        for h in range(GROUP):
            block = jnp.concatenate([out[h * 8:(h + 1) * 8] for out in outs], axis=0)
            e_buf[0, :, h * HD:(h + 1) * HD] = block.astype(BF16)

    def y_copies(view, send, recv):
        up, down = at_y(1), at_y(-1)
        plan = [(0, 3, 0, up), (0, 1, 1, down), (0, 3, 1, up), (0, 1, 0, down), (3, 2, 0, up), (1, 2, 1, down)]
        return [
            remote(view(src, half), view(dst, half), send.at[0], recv.at[sem], peer)
            for (src, dst, half, peer), sem in zip(plan, (0, 1, 2, 2, 3, 3))
        ]

    b_copies = y_copies(lambda slot, half: b_buf.at[slot, half * 512:(half + 1) * 512], b_send, b_recv)

    def forward(copies):
        for i in range(2):
            copies[i].wait_recv()
            copies[4 + i].start()

    def span(g):
        r, p0, n = GROUPS[g]
        return (r * 8 + p0) * NODES, n * NODES

    def multiply(g, rels=range(Y)):
        start, size = span(g)
        r, p0, n = GROUPS[g]
        left = a_buf[r, p0:p0 + n].reshape(size, 1024)
        for rel in rels:
            product = jnp.dot(left, b_buf[rel], preferred_element_type=F32).astype(BF16)
            part[2 * rel, start:start + size, :] = product[:, :128]
            part[2 * rel + 1, start:start + size, :] = product[:, 128:]
        if 2 in rels:
            pair_copy(g).start()

    def pair_copy(g):
        start, size = span(g)
        return remote(
            part.at[pl.ds((1 - c) * 4, 4), start:start + size], pair_in.at[:, start:start + size],
            d_send.at[0], d_recv.at[g], partner,
        )

    def r1_copy(g, way):
        start, size = span(g)
        half = slice(start + way * size // 2, start + (way + 1) * size // 2)
        return remote(
            pair.at[(x + 2) % X, half], r1_in.at[half], r1_send.at[0], r1_recv.at[g], at_x(1 - 2 * way)
        )

    def add_pair(g):
        start, size = span(g)
        rows = slice(start, start + size)
        pair_copy(g).wait_recv()
        for i in range(X):
            pair[i, rows, :] = (part[c * 4 + i, rows, :].astype(F32) + pair_in[i, rows, :].astype(F32)).astype(BF16)
        for way in range(2):
            r1_copy(g, way).start()

    def r2_copy(g, way):
        start, size = span(g)
        rows = slice(start, start + size)
        return remote(
            r2_src.at[way, rows], r2_in.at[way, rows], r2_send.at[0], r2_recv.at[g], at_x(1 - 2 * way)
        )

    def add_far(g):
        start, size = span(g)
        received(r1_in.at[start:start + size], r1_recv.at[g])
        for way in range(2):
            near = (x + 1 - 2 * way + X) % X
            for half in range(2):
                rows = slice(start + half * size // 2, start + (half + 1) * size // 2)
                value = pair[near, rows, :]
                if half == way:
                    value = (value.astype(F32) + r1_in[rows, :].astype(F32)).astype(BF16)
                r2_src[way, rows, :] = value
            r2_copy(g, way).start()

    part_of = c * 4 + x
    own_slice = ((y + part_of // 2) % Y) * 2 + part_of % 2

    def t_copy(r, p):
        return remote(
            red.at[r * 8 + p], fin.at[own_slice, r], t_send.at[0], t_recv.at[r],
            (((z + OFFSET[p] + Z) % Z) * Y + y, z),
        )

    def deliver(copy, p, keep):
        if p == 0:
            pl.when(jnp.logical_not(is_self))(lambda: copy(p).start())
            pl.when(is_self)(keep)
        else:
            copy(p).start()

    def spread(g):
        start, size = span(g)
        rows = slice(start, start + size)
        received(r2_in.at[:, start:start + size], r2_recv.at[g])
        total = pair[x, rows, :].astype(F32) + r2_in[0, rows, :].astype(F32) + r2_in[1, rows, :].astype(F32)
        total = total.astype(BF16)
        r, p0, n = GROUPS[g]
        red[r * 8 + p0:r * 8 + p0 + n] = total.reshape(n, NODES, HD)

        def keep():
            fin[own_slice, r] = red[r * 8]

        for p in range(p0, p0 + n):
            deliver(functools.partial(t_copy, r), p, keep)

    def finish(r):
        rows = slice(r * NODES, (r + 1) * NODES)
        pl.when(jnp.logical_not(is_self))(lambda: received(fin.at[:, r], t_recv.at[r]))
        pl.when(is_self)(lambda: received(fin.at[0:7, r], t_recv.at[r]))
        for i in range(8):
            cols = slice(i * HD, (i + 1) * HD)
            hid_out[rows, cols] = (res[rows, cols].astype(F32) + fin[i, r].astype(F32)).astype(BF16)

    def bufs(g):
        return rows_e, 0, 0, 8

    def e_multiply(g, rels=range(Y)):
        (part, *_), r, n0, n1 = bufs(g)
        size = part.shape[-2]
        left = e_buf[...].reshape(8 * size, 1024)
        for rel in rels:
            product = jnp.dot(left, b_buf[rel], preferred_element_type=F32).astype(BF16)
            for p in range(8):
                block = (z + OFFSET[p] + Z) % Z
                for half in range(2):
                    part[r, block // 2, block % 2, 2 * rel + half] = product[
                        p * size:(p + 1) * size, half * 128:half * 128 + 128
                    ]
        if 2 in rels:
            e_pair_copy(g).start()

    def e_pair_copy(g):
        (part, pair_in, *_), r, n0, n1 = bufs(g)
        return remote(
            part.at[r, :, 1 - c, n0:n1], pair_in.at[r, :, n0:n1], d_send.at[1], d_recv.at[g], partner
        )

    def e_r1_copy(g, way):
        (_, _, pair, r1_in, *_), r, n0, n1 = bufs(g)
        n = (n1 - n0) // 2
        half = slice(n0 + way * n, n0 + way * n + n)
        return remote(
            pair.at[r, (x + 2) % X, half], r1_in.at[r, half], r1_send.at[1], r1_recv.at[g],
            at_x(1 - 2 * way),
        )

    def e_add_pair(g):
        (part, pair_in, pair, *_), r, n0, n1 = bufs(g)
        e_pair_copy(g).wait_recv()
        for i in range(X):
            pair[r, i, n0:n1] = (part[r, i, c, n0:n1].astype(F32) + pair_in[r, i, n0:n1].astype(F32)).astype(BF16)
        for way in range(2):
            e_r1_copy(g, way).start()

    def e_r2_copy(g, way):
        (_, _, _, _, r2_src, r2_in, *_), r, n0, n1 = bufs(g)
        return remote(
            r2_src.at[way, r, n0:n1], r2_in.at[way, r, n0:n1], r2_send.at[1], r2_recv.at[g],
            at_x(1 - 2 * way),
        )

    def e_add_far(g):
        (_, _, pair, r1_in, r2_src, *_), r, n0, n1 = bufs(g)
        n = (n1 - n0) // 2
        received(r1_in.at[r, n0:n1], r1_recv.at[g])
        for way in range(2):
            near = (x + 1 - 2 * way + X) % X
            for half in range(2):
                part_n = slice(n0 + half * n, n0 + half * n + n)
                value = pair[r, near, part_n]
                if half == way:
                    value = (value.astype(F32) + r1_in[r, part_n].astype(F32)).astype(BF16)
                r2_src[way, r, part_n] = value
            e_r2_copy(g, way).start()

    def e_t_copy(g):
        (*_, red, fin), r, n0, n1 = bufs(g)
        return remote(red.at[r, n0:n1], fin.at[r, n0:n1], et_send.at[0], et_recv.at[0], (m * Y + y, z))

    def e_spread(g):
        (_, _, pair, _, _, r2_in, red, fin), r, n0, n1 = bufs(g)
        received(r2_in.at[:, r, n0:n1], r2_recv.at[g])
        total = pair[r, x, n0:n1].astype(F32) + r2_in[0, r, n0:n1].astype(F32) + r2_in[1, r, n0:n1].astype(F32)
        red[r, n0:n1] = total.astype(BF16)
        pl.when(jnp.logical_not(is_self))(lambda: e_t_copy(g).start())

        @pl.when(is_self)
        def _():
            fin[r, n0:n1] = red[r, n0:n1]

    def e_t_wait(g):
        pl.when(jnp.logical_not(is_self))(lambda: e_t_copy(g).wait_recv())

    def e_summed(g, i):
        (*_, fin), r, _, _ = bufs(g)
        return fin[r, ((i // 2 - y + Y) % Y) * 2 + i % 2].astype(F32)

    def cz_copy(s, way):
        sign = 1 if way == 0 else -1
        src = 0 if s == 1 else 2 * (s - 1) - 1 + way
        dst = 2 * s - 1 + way
        return remote(
            c_buf.at[src, y], c_buf.at[dst, y], cz_send.at[0], cz_recv.at[s - 1, way], at_z(sign)
        )

    def cd_copy(way, i, dy, from_y):
        sign = 1 if way == 0 else -1
        cut = slice(512 * way, 512 * way + 512)
        peer = (((z + sign + Z) % Z) * Y + (y + dy) % Y, m)
        return remote(
            c_buf.at[5 + way, from_y, :, cut], c_buf.at[7, from_y, :, cut], cd_send.at[0],
            cd_recv.at[0], peer,
        )

    def cy_copy(part, i):
        slots = slice(*PARTS[part])
        if i < 2:
            return remote(
                c_buf.at[slots, y], c_buf.at[slots, y], cy_send.at[0], cy_recv.at[2 * part + i], at_y(1 - 2 * i)
            )
        way = i - 2
        src = (y - 1 + 2 * way + Y) % Y
        block = c_buf.at[slots, src, :, 512 * way:512 * way + 512]
        return remote(block, block, cy_send.at[0], cy_recv.at[6 + part], at_y(1 - 2 * way))

    def c_start():
        rows = [picked(r, res[r * NODES:(r + 1) * NODES, :]) for r in range(2)]
        rows = jnp.concatenate(rows, axis=0)
        e_t_wait(EXTRA)
        for i in range(8):
            cols = slice(i * HD, (i + 1) * HD)
            c_buf[0, y, :, cols] = (rows[:, cols] + e_summed(EXTRA, i)).astype(BF16)
        for way in range(2):
            cz_copy(1, way).start()

    def c_go(s):
        for way in range(2):
            cz_copy(s, way).wait_recv()
            if s < 3:
                cz_copy(s + 1, way).start()
            else:
                for dy in range(Y):
                    cd_copy(way, dy, dy, y).start()
        for i in range(2):
            cy_copy(s - 1, i).start()

    def c_relay(part):
        for way in range(2):
            cy_copy(part, way).wait_recv()
            cy_copy(part, 2 + way).start()

    def c_end(part):
        received(c_buf.at[slice(*PARTS[part]), 0], cy_recv.at[6 + part])
        if part == 2:
            received(c_buf.at[0], cd_recv.at[0])
            acc_out[(z + 4) % Z] = c_buf[7]
        for p in range(*PARTS[part]):
            acc_out[(z + OFFSET[p] + Z) % Z] = c_buf[p]

    local["par"].wait()
    local["acn"].wait()
    reach = ancestors()
    pl.semaphore_wait(barrier, 7)
    local["w"].wait()
    for i in range(4):
        b_copies[i].start()
    for name in ("lens", "q", "tk", "tv", "k0", "k1", "v0", "v1"):
        local[name].wait()
    e_attend(reach)
    e_go(1)
    absorb(0, 0)
    absorb(0, 1)
    e_go(2)
    close(0, reach)
    a_go(0, 1)
    absorb(1, 0)
    forward(b_copies)
    absorb(1, 1)
    e_go(3)
    close(1, reach)
    a_go(1, 1)
    e_go(4)
    a_go(0, 2)
    a_go(1, 2)
    e_end()
    received(b_buf.at[0], b_recv.at[2])
    e_multiply(EXTRA, (0, 1, 3))
    a_go(0, 3)
    received(b_buf.at[0], b_recv.at[3])
    e_multiply(EXTRA, (2,))
    multiply(0)
    a_go(1, 3)
    e_add_pair(EXTRA)
    multiply(1)
    add_pair(0)
    a_go(0, 4)
    e_add_far(EXTRA)
    add_pair(1)
    a_go(1, 4)
    add_far(0)
    e_spread(EXTRA)
    add_far(1)
    a_end(0)
    multiply(2)
    a_end(1)
    multiply(3)
    spread(0)
    add_pair(2)
    local["res"].wait()
    c_start()
    spread(1)
    add_pair(3)
    c_go(1)
    add_far(2)
    add_far(3)
    c_go(2)
    c_relay(0)
    spread(2)
    spread(3)
    c_go(3)
    c_relay(1)
    c_relay(2)
    c_end(0)
    c_end(1)
    finish(0)
    finish(1)
    c_end(2)

    drained(a_buf.at[:, 0:7], a_send.at[0])
    drained(e_buf.at[0:7], e_send.at[0])
    drained(b_buf.at[0:3], b_send.at[0])
    drained(pair_in, d_send.at[0])
    drained(r1_in, r1_send.at[0])
    drained(r2_in, r2_send.at[0])
    e_pair_copy(EXTRA).wait_send()
    drained(rows_e[3], r1_send.at[1])
    drained(rows_e[5], r2_send.at[1])
    drained(c_buf.at[0:3, 0:2], cz_send.at[0])
    drained(c_buf.at[0:7, 0:3], cy_send.at[0])
    drained(c_buf.at[0], cd_send.at[0])

    @pl.when(jnp.logical_not(is_self))
    def _():
        drained(fin, t_send.at[0])
        e_t_copy(EXTRA).wait_send()

    pl.when(is_self)(lambda: drained(fin.at[0:7], t_send.at[0]))


def per_device(
    queries, tree_keys, tree_values, cache_keys, cache_values, cache_lens, parents, accepted_nodes, residual, out_weight
):
    vmem = pl.BlockSpec(memory_space=pltpu.VMEM)
    hbm = pl.BlockSpec(memory_space=pl.ANY)
    sems = pltpu.SemaphoreType.DMA
    groups = len(GROUPS) + 1

    def summing(count, size):
        shapes = [
            (count, X, 2, 8), (count, X, 8), (count, X, 8), (count, 8), (2, count, 8), (2, count, 8), (count, 8),
            (count, 8),
        ]
        return [pltpu.VMEM((*dims, size, HD), BF16) for dims in shapes]

    hidden, accepted = pl.pallas_call(
        kernel,
        out_shape=(
            pltpu.VMEM((128, 1024), BF16),
            pltpu.VMEM((Z, Y, 16, 1024), BF16),
        ),
        in_specs=[hbm] * 10,
        out_specs=(vmem, vmem),
        scratch_shapes=[
            pltpu.SMEM((2,), jnp.int32),
            pltpu.VMEM((2, NODES), jnp.int32),
            pltpu.VMEM((2, 8), jnp.int32),
            pltpu.VMEM((128, 1024), BF16),
            pltpu.VMEM((128, HD), BF16),
            pltpu.VMEM((128, HD), BF16),
            pltpu.VMEM((2, CACHE, HD), BF16),
            pltpu.VMEM((2, CACHE, HD), BF16),
            pltpu.VMEM((512, 128), F32),
            pltpu.VMEM((512, 128), F32),
            pltpu.VMEM((512, 128), F32),
            pltpu.VMEM((2, 8, NODES, 1024), BF16),
            pltpu.VMEM((8, 16, 1024), BF16),
            pltpu.VMEM((Y, 1024, 256), BF16),
            pltpu.VMEM((8, 1024, 128), BF16),
            pltpu.VMEM((4, 1024, 128), BF16),
            pltpu.VMEM((4, 1024, 128), BF16),
            pltpu.VMEM((1024, 128), BF16),
            pltpu.VMEM((2, 1024, 128), BF16),
            pltpu.VMEM((2, 1024, 128), BF16),
            pltpu.VMEM((16, NODES, HD), BF16),
            pltpu.VMEM((8, 2, NODES, HD), BF16),
            summing(1, 16),
            pltpu.VMEM((8, Y, 16, 1024), BF16),
            pltpu.VMEM((128, 1024), BF16),
            sems((12,)),
            sems((1,)), sems((2, 4, 2)),
            sems((1,)), sems((4, 2)),
            sems((1,)), sems((4,)),
            sems((2,)), sems((groups,)),
            sems((2,)), sems((groups,)),
            sems((2,)), sems((groups,)),
            sems((1,)), sems((2,)),
            sems((1,)), sems((1,)),
            sems((1,)), sems((3, 2)),
            sems((1,)), sems((9,)),
            sems((1,)), sems((1,)),
        ],
        compiler_params=pltpu.CompilerParams(
            collective_id=0, has_side_effects=True, vmem_limit_bytes=60000 * 1024
        ),
        name="verify",
    )(
        cache_lens, parents, accepted_nodes, queries, tree_keys, tree_values, cache_keys, cache_values, residual,
        out_weight,
    )
    return hidden, accepted.reshape(512, 1024)


def solution(mesh):
    placed = (
        P("dp", "mp"),
        P("dp", "mp"),
        P("dp", "mp"),
        P("dp", None, "mp"),
        P("dp", None, "mp"),
        P("dp"),
        P("dp", None),
        P("dp", None),
        P("dp", "mp"),
        P("mp", "dp"),
    )
    return jax.shard_map(
        per_device,
        mesh=mesh,
        in_specs=placed,
        out_specs=(P("dp", "mp"), P(None, "mp")),
        check_vma=False,
    )
```

```python
import functools
import math

import jax
import jax.numpy as jnp
from jax import lax
from jax.experimental import pallas as pl
from jax.experimental.pallas import tpu as pltpu
from jax.sharding import PartitionSpec as P

F32, BF16 = jnp.float32, jnp.bfloat16
MESH = pl.DeviceIdType.MESH
Z, Y, X = 8, 4, 4
NODES, HD, GROUP = 64, 128, 8
SCALE = math.log2(math.e) / math.sqrt(HD)
NEG = -1e30
NT = (((1,), (1,)), ((), ()))
TN = (((0,), (0,)), ((), ()))
CHUNK = 2048
ROWS = 256
CACHE = 4096
OFFSET = (0, -1, 1, -2, 2, -3, 3, 4)
GROUPS = ((0, 0, 4), (1, 0, 4), (0, 4, 4), (1, 4, 4))
EXTRA = len(GROUPS)
PARTS = ((0, 3), (3, 5))


def kernel(
    lens_hbm, par_hbm, acn_hbm, q_hbm, tk_hbm, tv_hbm, k_hbm, v_hbm, res_hbm, w_hbm,
    hid_out, acc_out,
    lens, par, acn, q, tk, tv, kb, vb, m_s, l_s, acc_s, a_buf, e_buf, b_buf, part, pair_in, pair, r1_in, r2_src, r2_in, red, mid, fin,
    rows_e, c_buf, res,
    loc_sem, a_send, a_recv, e_send, e_recv, b_send, b_recv, d_send, d_recv, r1_send, r1_recv, r2_send, r2_recv,
    t_send, t_recv, u_send, u_recv, et_send, et_recv, cz_send, cz_recv, cy_send, cy_recv,
    cd_send, cd_recv,
):
    dp, m = lax.axis_index("dp"), lax.axis_index("mp")
    z, y = dp // Y, dp % Y
    x, c = m // 2, m % 2
    is_self = m == z

    def at_z(dz):
        return (((z + dz + Z) % Z) * Y + y, m)

    def at_y(dy):
        return (z * Y + (y + dy + Y) % Y, m)

    def at_x(dx):
        return (dp, ((x + dx + X) % X) * 2 + c)

    partner = (dp, x * 2 + (1 - c))

    barrier = pltpu.get_barrier_semaphore()

    def greet(peer):
        pl.semaphore_signal(barrier, inc=1, device_id=peer, device_id_type=MESH)

    for peer in [at_y(1), at_y(-1), at_z(1), at_z(-1), partner, at_x(1), at_x(-1)]:
        greet(peer)
    local = {}
    for i, (name, src, dst) in enumerate(
        [("w", w_hbm, b_buf.at[0]), ("par", par_hbm, par), ("acn", acn_hbm, acn), ("lens", lens_hbm, lens),
         ("q", q_hbm, q), ("tk", tk_hbm, tk), ("tv", tv_hbm, tv), ("k0", k_hbm.at[0], kb.at[0]),
         ("k1", k_hbm.at[1], kb.at[1]), ("v0", v_hbm.at[0], vb.at[0]), ("v1", v_hbm.at[1], vb.at[1]),
         ("res", res_hbm, res)]
    ):
        local[name] = pltpu.make_async_copy(src, dst, loc_sem.at[i])
        local[name].start()

    def remote(src, dst, send, recv, peer):
        return pltpu.make_async_remote_copy(
            src_ref=src, dst_ref=dst, send_sem=send, recv_sem=recv, device_id=peer, device_id_type=MESH
        )

    def drained(view, sem):
        remote(view, view, sem, sem, partner).wait_send()

    def received(view, sem):
        remote(view, view, sem, sem, partner).wait_recv()

    def ancestors():
        sub = lax.broadcasted_iota(jnp.int32, (NODES, NODES), 0)
        lane = lax.broadcasted_iota(jnp.int32, (NODES, NODES), 1)
        eye = jnp.where(sub == lane, 1.0, 0.0)
        reach = [jnp.where(sub == par[r:r + 1, :], 1.0, 0.0) + eye for r in range(2)]
        for _ in range(6):
            step = [one.astype(BF16) for one in reach]
            reach = [jnp.minimum(jnp.dot(one, one, preferred_element_type=F32), 1.0) for one in step]
        sub = lax.broadcasted_iota(jnp.int32, (NODES, 128), 0)
        lane = lax.broadcasted_iota(jnp.int32, (NODES, 128), 1)
        return [
            lax.dot_general(
                reach[r].astype(BF16), jnp.where(sub + r * NODES == lane, 1.0, 0.0).astype(BF16), TN,
                preferred_element_type=F32,
            )
            for r in range(2)
        ]

    def picked(r, rows):
        nodes = lax.broadcasted_iota(jnp.int32, (NODES, 8), 0)
        pick = jnp.where(nodes == acn[r:r + 1, :], 1.0, 0.0).astype(BF16)
        return lax.dot_general(pick, rows, TN, preferred_element_type=F32)

    heads = ROWS // NODES

    def query_rows(r, b):
        return jnp.concatenate(
            [q[r * NODES:(r + 1) * NODES, h * HD:(h + 1) * HD] for h in range(b * heads, (b + 1) * heads)], axis=0
        )

    def absorb(r, j):
        count = lens[r]
        base = j * CHUNK
        keys = kb[r, base:base + CHUNK, :]
        values = vb[r, base:base + CHUNK, :]
        first = j == 0
        live = (lax.broadcasted_iota(jnp.int32, (1, CHUNK), 1) + base) < count
        bias = jnp.where(live, 0.0, NEG)
        for b in range(512 // ROWS):
            rows = slice(b * ROWS, (b + 1) * ROWS)
            s = lax.dot_general(query_rows(r, b), keys, NT, preferred_element_type=F32) * SCALE
            cols = [slice(t * 128, (t + 1) * 128) for t in range(CHUNK // 128)]
            scores = [s[:, t] if base + t.stop <= 1024 else s[:, t] + bias[:, t] for t in cols]
            top = functools.reduce(jnp.maximum, scores)
            new = jnp.broadcast_to(jnp.max(top, axis=1, keepdims=True), (ROWS, 128))
            if not first:
                old = m_s[rows, :]
                new = jnp.maximum(old, new)
                rescale = jnp.exp2(old - new)
            m_s[rows, :] = new
            weights = [jnp.exp2(one - new) for one in scores]
            total = functools.reduce(jnp.add, weights)
            out = jnp.dot(
                jnp.concatenate([one.astype(BF16) for one in weights], axis=1), values, preferred_element_type=F32
            )
            l_s[rows, :] = total if first else l_s[rows, :] * rescale + total
            acc_s[rows, :] = out if first else acc_s[rows, :] * rescale + out

    def close(r, reach):
        mask = jnp.concatenate([reach[r] > 0.5] * heads, axis=0)
        for b in range(512 // ROWS):
            rows = slice(b * ROWS, (b + 1) * ROWS)
            s = lax.dot_general(query_rows(r, b), tk[...], NT, preferred_element_type=F32) * SCALE
            s = jnp.where(mask, s, NEG)
            old = m_s[rows, :]
            new = jnp.maximum(old, jnp.broadcast_to(jnp.max(s, axis=1, keepdims=True), (ROWS, 128)))
            rescale = jnp.exp2(old - new)
            p = jnp.exp2(s - new)
            total = jnp.sum(l_s[rows, :] * rescale + p, axis=1, keepdims=True)
            out = acc_s[rows, :] * rescale + jnp.dot(p.astype(BF16), tv[...], preferred_element_type=F32)
            out = (out / total).astype(BF16)
            for h in range(heads):
                col = (b * heads + h) * HD
                a_buf[r, 0, :, col:col + HD] = out[h * NODES:(h + 1) * NODES, :]

    def a_copy(r, s, way):
        sign = 1 if way == 0 else -1
        src = 0 if s == 1 else 2 * (s - 1) - 1 + way
        if s < 4:
            dst, cut = 2 * s - 1 + way, slice(None)
        else:
            dst, cut = 7, slice(32 * way, 32 * way + 32)
        return remote(
            a_buf.at[r, src, cut], a_buf.at[r, dst, cut], a_send.at[0], a_recv.at[r, s - 1, way], at_z(sign)
        )

    def a_go(r, s):
        for way in range(2):
            if s > 1:
                a_copy(r, s - 1, way).wait_recv()
            a_copy(r, s, way).start()

    def a_end(r):
        for way in range(2):
            a_copy(r, 4, way).wait_recv()

    def e_copy(s, way):
        sign = 1 if way == 0 else -1
        src = 0 if s == 1 else 2 * (s - 1) - 1 + way
        if s < 4:
            dst, cut = 2 * s - 1 + way, slice(None)
        else:
            dst, cut = 7, slice(512 * way, 512 * way + 512)
        return remote(
            e_buf.at[src, :, cut], e_buf.at[dst, :, cut], e_send.at[0], e_recv.at[s - 1, way], at_z(sign)
        )

    def e_go(s):
        for way in range(2):
            if s > 1:
                e_copy(s - 1, way).wait_recv()
            e_copy(s, way).start()

    def e_end():
        for way in range(2):
            e_copy(4, way).wait_recv()

    def e_attend(reach):
        outs = []
        for r in range(2):
            chosen = picked(r, q[r * NODES:(r + 1) * NODES, :])
            rows = jnp.concatenate([chosen[:, h * HD:(h + 1) * HD] for h in range(GROUP)], axis=0).astype(BF16)
            mask = jnp.concatenate([picked(r, reach[r].astype(BF16))] * GROUP, axis=0) > 0.5
            tree = lax.dot_general(rows, tk[...], NT, preferred_element_type=F32) * SCALE
            tree = jnp.where(mask, tree, NEG)
            s = lax.dot_general(rows, kb[r], NT, preferred_element_type=F32) * SCALE
            live = lax.broadcasted_iota(jnp.int32, (1, CACHE), 1) < lens[r]
            s = s + jnp.where(live, 0.0, NEG)
            cols = [s[:, t * 128:(t + 1) * 128] for t in range(CACHE // 128)]
            top = jnp.max(functools.reduce(jnp.maximum, cols + [tree]), axis=1, keepdims=True)
            weights = [jnp.exp2(one - top) for one in cols]
            first = jnp.exp2(tree - top)
            total = jnp.sum(functools.reduce(jnp.add, weights + [first]), axis=1, keepdims=True)
            out = jnp.dot(first.astype(BF16), tv[...], preferred_element_type=F32) + jnp.dot(
                jnp.concatenate([one.astype(BF16) for one in weights], axis=1), vb[r], preferred_element_type=F32
            )
            outs.append(out / total)
        for h in range(GROUP):
            block = jnp.concatenate([out[h * 8:(h + 1) * 8] for out in outs], axis=0)
            e_buf[0, :, h * HD:(h + 1) * HD] = block.astype(BF16)

    def y_copies(view, send, recv):
        up, down = at_y(1), at_y(-1)
        plan = [(0, 3, 0, up), (0, 1, 1, down), (0, 3, 1, up), (0, 1, 0, down), (3, 2, 0, up), (1, 2, 1, down)]
        return [
            remote(view(src, half), view(dst, half), send.at[0], recv.at[sem], peer)
            for (src, dst, half, peer), sem in zip(plan, (0, 1, 2, 2, 3, 3))
        ]

    b_copies = y_copies(lambda slot, half: b_buf.at[slot, half * 512:(half + 1) * 512], b_send, b_recv)

    def forward(copies):
        for i in range(2):
            copies[i].wait_recv()
            copies[4 + i].start()

    def span(g):
        r, p0, n = GROUPS[g]
        return (r * 8 + p0) * NODES, n * NODES

    def multiply(g, rels=range(Y)):
        start, size = span(g)
        r, p0, n = GROUPS[g]
        left = a_buf[r, p0:p0 + n].reshape(size, 1024)
        for rel in rels:
            product = jnp.dot(left, b_buf[rel], preferred_element_type=F32).astype(BF16)
            part[2 * rel, start:start + size, :] = product[:, :128]
            part[2 * rel + 1, start:start + size, :] = product[:, 128:]
        if 2 in rels:
            pair_copy(g).start()

    def pair_copy(g):
        start, size = span(g)
        return remote(
            part.at[pl.ds((1 - c) * 4, 4), start:start + size], pair_in.at[:, start:start + size],
            d_send.at[0], d_recv.at[g], partner,
        )

    def r1_copy(g, way):
        start, size = span(g)
        half = slice(start + way * size // 2, start + (way + 1) * size // 2)
        return remote(
            pair.at[(x + 2) % X, half], r1_in.at[half], r1_send.at[0], r1_recv.at[g], at_x(1 - 2 * way)
        )

    def add_pair(g):
        start, size = span(g)
        rows = slice(start, start + size)
        pair_copy(g).wait_recv()
        for i in range(X):
            pair[i, rows, :] = (part[c * 4 + i, rows, :].astype(F32) + pair_in[i, rows, :].astype(F32)).astype(BF16)
        for way in range(2):
            r1_copy(g, way).start()

    def r2_copy(g, way):
        start, size = span(g)
        rows = slice(start, start + size)
        return remote(
            r2_src.at[way, rows], r2_in.at[way, rows], r2_send.at[0], r2_recv.at[g], at_x(1 - 2 * way)
        )

    def add_far(g):
        start, size = span(g)
        received(r1_in.at[start:start + size], r1_recv.at[g])
        for way in range(2):
            near = (x + 1 - 2 * way + X) % X
            for half in range(2):
                rows = slice(start + half * size // 2, start + (half + 1) * size // 2)
                value = pair[near, rows, :]
                if half == way:
                    value = (value.astype(F32) + r1_in[rows, :].astype(F32)).astype(BF16)
                r2_src[way, rows, :] = value
            r2_copy(g, way).start()

    part_of = c * 4 + x
    own_slice = ((y + part_of // 2) % Y) * 2 + part_of % 2

    def t_copy(r, p):
        if p < 4:
            return remote(red.at[r * 8 + p], mid.at[z, r], t_send.at[0], t_recv.at[r], at_z(OFFSET[p]))
        peer = (((z + OFFSET[p] + Z) % Z) * Y + y, z)
        return remote(red.at[r * 8 + p], fin.at[own_slice, r], t_send.at[0], u_recv.at[r], peer)

    def u_copy(r, p):
        block = (z - OFFSET[p] + Z) % Z
        return remote(mid.at[block, r], fin.at[own_slice, r], u_send.at[0], u_recv.at[r], (dp, block))

    def onward(r):
        received(fin.at[0:3, r], t_recv.at[r])
        for p in range(4):
            block = (z - OFFSET[p] + Z) % Z

            @pl.when(block == m)
            def _():
                fin[own_slice, r] = mid[block, r]

            @pl.when(block != m)
            def _():
                u_copy(r, p).start()

    gap = (z - m + Z) % Z
    far = jnp.logical_and(gap >= 2, gap <= 5)

    def spread(g):
        start, size = span(g)
        rows = slice(start, start + size)
        received(r2_in.at[:, start:start + size], r2_recv.at[g])
        total = pair[x, rows, :].astype(F32) + r2_in[0, rows, :].astype(F32) + r2_in[1, rows, :].astype(F32)
        total = total.astype(BF16)
        r, p0, n = GROUPS[g]
        red[r * 8 + p0:r * 8 + p0 + n] = total.reshape(n, NODES, HD)

        for p in reversed(range(p0, p0 + n)):
            if p == 0:
                mid[z, r] = red[r * 8]
            else:
                t_copy(r, p).start()

    def finish(r):
        rows = slice(r * NODES, (r + 1) * NODES)
        pl.when(far)(lambda: received(fin.at[:, r], u_recv.at[r]))
        pl.when(jnp.logical_not(far))(lambda: received(fin.at[0:7, r], u_recv.at[r]))
        for i in range(8):
            cols = slice(i * HD, (i + 1) * HD)
            hid_out[rows, cols] = (res[rows, cols].astype(F32) + fin[i, r].astype(F32)).astype(BF16)

    def bufs(g):
        return rows_e, 0, 0, 8

    def e_multiply(g, rels=range(Y)):
        (part, *_), r, n0, n1 = bufs(g)
        size = part.shape[-2]
        left = e_buf[...].reshape(8 * size, 1024)
        for rel in rels:
            product = jnp.dot(left, b_buf[rel], preferred_element_type=F32).astype(BF16)
            for p in range(8):
                block = (z + OFFSET[p] + Z) % Z
                for half in range(2):
                    part[r, block // 2, block % 2, 2 * rel + half] = product[
                        p * size:(p + 1) * size, half * 128:half * 128 + 128
                    ]
        if 2 in rels:
            e_pair_copy(g).start()

    def e_pair_copy(g):
        (part, pair_in, *_), r, n0, n1 = bufs(g)
        return remote(
            part.at[r, :, 1 - c, n0:n1], pair_in.at[r, :, n0:n1], d_send.at[1], d_recv.at[g], partner
        )

    def e_r1_copy(g, way):
        (_, _, pair, r1_in, *_), r, n0, n1 = bufs(g)
        n = (n1 - n0) // 2
        half = slice(n0 + way * n, n0 + way * n + n)
        return remote(
            pair.at[r, (x + 2) % X, half], r1_in.at[r, half], r1_send.at[1], r1_recv.at[g],
            at_x(1 - 2 * way),
        )

    def e_add_pair(g):
        (part, pair_in, pair, *_), r, n0, n1 = bufs(g)
        e_pair_copy(g).wait_recv()
        for i in range(X):
            pair[r, i, n0:n1] = (part[r, i, c, n0:n1].astype(F32) + pair_in[r, i, n0:n1].astype(F32)).astype(BF16)
        for way in range(2):
            e_r1_copy(g, way).start()

    def e_r2_copy(g, way):
        (_, _, _, _, r2_src, r2_in, *_), r, n0, n1 = bufs(g)
        return remote(
            r2_src.at[way, r, n0:n1], r2_in.at[way, r, n0:n1], r2_send.at[1], r2_recv.at[g],
            at_x(1 - 2 * way),
        )

    def e_add_far(g):
        (_, _, pair, r1_in, r2_src, *_), r, n0, n1 = bufs(g)
        n = (n1 - n0) // 2
        received(r1_in.at[r, n0:n1], r1_recv.at[g])
        for way in range(2):
            near = (x + 1 - 2 * way + X) % X
            for half in range(2):
                part_n = slice(n0 + half * n, n0 + half * n + n)
                value = pair[r, near, part_n]
                if half == way:
                    value = (value.astype(F32) + r1_in[r, part_n].astype(F32)).astype(BF16)
                r2_src[way, r, part_n] = value
            e_r2_copy(g, way).start()

    def e_t_copy(g):
        (*_, red, fin), r, n0, n1 = bufs(g)
        return remote(red.at[r, n0:n1], fin.at[r, n0:n1], et_send.at[0], et_recv.at[0], (m * Y + y, z))

    def e_spread(g):
        (_, _, pair, _, _, r2_in, red, fin), r, n0, n1 = bufs(g)
        received(r2_in.at[:, r, n0:n1], r2_recv.at[g])
        total = pair[r, x, n0:n1].astype(F32) + r2_in[0, r, n0:n1].astype(F32) + r2_in[1, r, n0:n1].astype(F32)
        red[r, n0:n1] = total.astype(BF16)
        pl.when(jnp.logical_not(is_self))(lambda: e_t_copy(g).start())

        @pl.when(is_self)
        def _():
            fin[r, n0:n1] = red[r, n0:n1]

    def e_t_wait(g):
        pl.when(jnp.logical_not(is_self))(lambda: e_t_copy(g).wait_recv())

    def e_summed(g, i):
        (*_, fin), r, _, _ = bufs(g)
        return fin[r, ((i // 2 - y + Y) % Y) * 2 + i % 2].astype(F32)

    def cz_copy(s, way):
        sign = 1 if way == 0 else -1
        src = 0 if s == 1 else 2 * (s - 1) - 1 + way
        dst = 2 * s - 1 + way
        return remote(
            c_buf.at[src, y], c_buf.at[dst, y], cz_send.at[0], cz_recv.at[s - 1, way], at_z(sign)
        )

    def cd_copy(way, s, dy):
        sign = 1 if way == 0 else -1
        peer = (((z + sign + Z) % Z) * Y + (y + dy) % Y, m)
        if s == 3:
            recv = cz_recv.at[2, way] if dy == 0 else cd_recv.at[1]
            return remote(c_buf.at[3 + way, y], c_buf.at[5 + way, y], cz_send.at[0], recv, peer)
        cut = slice(512 * way, 512 * way + 512)
        return remote(
            c_buf.at[5 + way, y, :, cut], c_buf.at[7, y, :, cut], cd_send.at[0], cd_recv.at[0], peer
        )

    def cy_copy(part, i):
        slots = slice(*PARTS[part])
        if i < 2:
            return remote(
                c_buf.at[slots, y], c_buf.at[slots, y], cy_send.at[0], cy_recv.at[2 * part + i], at_y(1 - 2 * i)
            )
        way = i - 2
        src = (y - 1 + 2 * way + Y) % Y
        block = c_buf.at[slots, src, :, 512 * way:512 * way + 512]
        return remote(block, block, cy_send.at[0], cy_recv.at[4 + part], at_y(1 - 2 * way))

    def c_start():
        rows = [picked(r, res[r * NODES:(r + 1) * NODES, :]) for r in range(2)]
        rows = jnp.concatenate(rows, axis=0)
        e_t_wait(EXTRA)
        for i in range(8):
            cols = slice(i * HD, (i + 1) * HD)
            c_buf[0, y, :, cols] = (rows[:, cols] + e_summed(EXTRA, i)).astype(BF16)
        for way in range(2):
            cz_copy(1, way).start()

    def c_go(s):
        for way in range(2):
            (cz_copy(s, way) if s < 3 else cd_copy(way, 3, 0)).wait_recv()
            (cz_copy(2, way) if s == 1 else cd_copy(way, s + 1, 0)).start()
        if s < 3:
            for i in range(2):
                cy_copy(s - 1, i).start()
        if s > 1:
            for dy in range(1, Y):
                for way in range(2):
                    cd_copy(way, s + 1, dy).start()

    def c_relay(part):
        for way in range(2):
            cy_copy(part, way).wait_recv()
            cy_copy(part, 2 + way).start()

    def c_end(part):
        received(c_buf.at[slice(*PARTS[part]), 0], cy_recv.at[4 + part])
        for p in range(*PARTS[part]):
            acc_out[(z + OFFSET[p] + Z) % Z] = c_buf[p]

    def c_last():
        received(c_buf.at[0:3, 0:2], cd_recv.at[1])
        received(c_buf.at[0], cd_recv.at[0])
        for p in range(5, 8):
            acc_out[(z + OFFSET[p] + Z) % Z] = c_buf[p]

    local["par"].wait()
    local["acn"].wait()
    reach = ancestors()
    pl.semaphore_wait(barrier, 7)
    local["w"].wait()
    for i in range(4):
        b_copies[i].start()
    for name in ("lens", "q", "tk", "tv", "k0", "k1", "v0", "v1"):
        local[name].wait()
    e_attend(reach)
    e_go(1)
    absorb(0, 0)
    absorb(0, 1)
    e_go(2)
    close(0, reach)
    a_go(0, 1)
    absorb(1, 0)
    forward(b_copies)
    absorb(1, 1)
    e_go(3)
    close(1, reach)
    a_go(1, 1)
    e_go(4)
    a_go(0, 2)
    a_go(1, 2)
    e_end()
    received(b_buf.at[0], b_recv.at[2])
    e_multiply(EXTRA, (0, 1, 3))
    a_go(0, 3)
    received(b_buf.at[0], b_recv.at[3])
    e_multiply(EXTRA, (2,))
    multiply(0)
    e_add_pair(EXTRA)
    a_go(1, 3)
    multiply(1)
    add_pair(0)
    e_add_far(EXTRA)
    a_go(0, 4)
    add_pair(1)
    add_far(0)
    e_spread(EXTRA)
    a_go(1, 4)
    add_far(1)
    a_end(0)
    multiply(2)
    a_end(1)
    multiply(3)
    local["res"].wait()
    c_start()
    spread(0)
    add_pair(2)
    spread(1)
    add_pair(3)
    c_go(1)
    add_far(2)
    add_far(3)
    onward(0)
    onward(1)
    c_go(2)
    spread(2)
    c_relay(0)
    spread(3)
    c_go(3)
    c_relay(1)
    c_end(0)
    c_end(1)
    finish(0)
    finish(1)
    c_last()

    drained(a_buf.at[:, 0:7], a_send.at[0])
    drained(e_buf.at[0:7], e_send.at[0])
    drained(b_buf.at[0:3], b_send.at[0])
    drained(pair_in, d_send.at[0])
    drained(r1_in, r1_send.at[0])
    drained(r2_in, r2_send.at[0])
    e_pair_copy(EXTRA).wait_send()
    drained(rows_e[3], r1_send.at[1])
    drained(rows_e[5], r2_send.at[1])
    drained(c_buf.at[0:3], cz_send.at[0])
    drained(c_buf.at[0:5, 0:3], cy_send.at[0])
    drained(c_buf.at[0], cd_send.at[0])

    drained(fin.at[0:7], t_send.at[0])
    pl.when(far)(lambda: drained(fin.at[0:4], u_send.at[0]))
    pl.when(jnp.logical_not(far))(lambda: drained(fin.at[0:3], u_send.at[0]))
    pl.when(jnp.logical_not(is_self))(lambda: e_t_copy(EXTRA).wait_send())


def per_device(
    queries, tree_keys, tree_values, cache_keys, cache_values, cache_lens, parents, accepted_nodes, residual, out_weight
):
    vmem = pl.BlockSpec(memory_space=pltpu.VMEM)
    hbm = pl.BlockSpec(memory_space=pl.ANY)
    sems = pltpu.SemaphoreType.DMA
    groups = len(GROUPS) + 1

    def summing(count, size):
        shapes = [
            (count, X, 2, 8), (count, X, 8), (count, X, 8), (count, 8), (2, count, 8), (2, count, 8), (count, 8),
            (count, 8),
        ]
        return [pltpu.VMEM((*dims, size, HD), BF16) for dims in shapes]

    hidden, accepted = pl.pallas_call(
        kernel,
        out_shape=(
            pltpu.VMEM((128, 1024), BF16),
            pltpu.VMEM((Z, Y, 16, 1024), BF16),
        ),
        in_specs=[hbm] * 10,
        out_specs=(vmem, vmem),
        scratch_shapes=[
            pltpu.SMEM((2,), jnp.int32),
            pltpu.VMEM((2, NODES), jnp.int32),
            pltpu.VMEM((2, 8), jnp.int32),
            pltpu.VMEM((128, 1024), BF16),
            pltpu.VMEM((128, HD), BF16),
            pltpu.VMEM((128, HD), BF16),
            pltpu.VMEM((2, CACHE, HD), BF16),
            pltpu.VMEM((2, CACHE, HD), BF16),
            pltpu.VMEM((512, 128), F32),
            pltpu.VMEM((512, 128), F32),
            pltpu.VMEM((512, 128), F32),
            pltpu.VMEM((2, 8, NODES, 1024), BF16),
            pltpu.VMEM((8, 16, 1024), BF16),
            pltpu.VMEM((Y, 1024, 256), BF16),
            pltpu.VMEM((8, 1024, 128), BF16),
            pltpu.VMEM((4, 1024, 128), BF16),
            pltpu.VMEM((4, 1024, 128), BF16),
            pltpu.VMEM((1024, 128), BF16),
            pltpu.VMEM((2, 1024, 128), BF16),
            pltpu.VMEM((2, 1024, 128), BF16),
            pltpu.VMEM((16, NODES, HD), BF16),
            pltpu.VMEM((8, 2, NODES, HD), BF16),
            pltpu.VMEM((8, 2, NODES, HD), BF16),
            summing(1, 16),
            pltpu.VMEM((8, Y, 16, 1024), BF16),
            pltpu.VMEM((128, 1024), BF16),
            sems((12,)),
            sems((1,)), sems((2, 4, 2)),
            sems((1,)), sems((4, 2)),
            sems((1,)), sems((4,)),
            sems((2,)), sems((groups,)),
            sems((2,)), sems((groups,)),
            sems((2,)), sems((groups,)),
            sems((1,)), sems((2,)),
            sems((1,)), sems((2,)),
            sems((1,)), sems((1,)),
            sems((1,)), sems((3, 2)),
            sems((1,)), sems((6,)),
            sems((1,)), sems((2,)),
        ],
        compiler_params=pltpu.CompilerParams(
            collective_id=0, has_side_effects=True, vmem_limit_bytes=60000 * 1024
        ),
        name="verify",
    )(
        cache_lens, parents, accepted_nodes, queries, tree_keys, tree_values, cache_keys, cache_values, residual,
        out_weight,
    )
    return hidden, accepted.reshape(512, 1024)


def solution(mesh):
    placed = (
        P("dp", "mp"),
        P("dp", "mp"),
        P("dp", "mp"),
        P("dp", None, "mp"),
        P("dp", None, "mp"),
        P("dp"),
        P("dp", None),
        P("dp", None),
        P("dp", "mp"),
        P("mp", "dp"),
    )
    return jax.shard_map(
        per_device,
        mesh=mesh,
        in_specs=placed,
        out_specs=(P("dp", "mp"), P(None, "mp")),
        check_vma=False,
    )
```
